32 devices in a mesh: dom: 8 (over z, y), rep: 4 (over x, core).
Axes of the slice: x: 2, y: 2, z: 4, core: 2. Of those that a mesh axis runs over, the one named last changes fastest.
Arguments:
- ns_shape: bfloat16 [64, 256], replicated, may hold values from -0.75 to 0.75
- nm_shape: bfloat16 [64, 256], replicated, may hold values from -0.75 to 0.75
- sec_disp: bfloat16 [64, 262144], P(None, ('dom', 'rep')), may hold values from -6 to 6
- mst_disp: bfloat16 [64, 262144], P(None, ('dom', 'rep')), may hold values from -6 to 6
- gap_offset: float32 [262144], P(('dom', 'rep')), may hold values from -6 to 6
- quad_weight: float32 [256], replicated, may hold values from 0.25 to 4
- jacobian: float32 [262144], P(('dom', 'rep')), may hold values from 0.0005 to 0.005
- segment_slot: int32 [262144], P(('dom', 'rep')), may hold values from 0 to 1279, as said below
- face_id: int32 [262144], P(('dom', 'rep')), may hold values from 0 to 1073741823
- search_rank: int32 [262144], P(('dom', 'rep')), may hold values from 0 to 3
- live_rows: int32 [32], P(('dom', 'rep')), may hold values from 1024 to 8192, as said below
Outputs:
- contact_force: bfloat16 [64, 262144], P(None, ('dom', 'rep'))
- seg_pen: float32 [8192], P('dom')
- seg_face: int32 [8192], P('dom')
- seg_gap: float32 [8192], P('dom')
- mean_gap: float32 [], replicated
The draws below stay inside these ranges and needn't reach their ends.
Inputs may be any that keep to these rules, and one draw needn't show every extreme that they name: `segment_slot`: A row's segment is (1024 times the dom index of its device plus its slot) modulo 8192; slots of 1024 or more reach the next dom index's first 256 segments. `live_rows`: entry b counts the live rows of the device with flat index b (dom-major); they are that device's first rows, the rest are padding; some device is full in every draw.
All inputs are finite; a program needn't handle non-finite values.
Results may differ from the reference program's by a relative error of at most 0.0055.
Values sent between devices are 32-bit elements; how exact they have to be, the bound alone decides.
A program may use at most 64 MiB of HBM per device.

```python
import math
import jax
import jax.numpy as jnp
from jax import lax

P_SIZE = 256
K = 64
ROWS_DEV = 8192
SEG_DEV = 1024
SPILL = 256
SEGS = 8192
ROWS = 262144
N_REP = 4
DEVICES = 32


def draw_live_rows(key, part):
    first_key = jax.random.fold_in(key, 11)
    second_key = jax.random.fold_in(key, 23)
    counts = jax.random.randint(first_key, (DEVICES,), ROWS_DEV // 8, ROWS_DEV + 1, dtype=jnp.int32)
    full_device = jax.random.randint(second_key, (), 0, DEVICES, dtype=jnp.int32)
    return jnp.where(jnp.arange(DEVICES, dtype=jnp.int32) == full_device, ROWS_DEV, counts).astype(jnp.int32)


def draw_segment_slot(key, part):
    window_len = SEG_DEV + SPILL
    dom_count = DEVICES // N_REP
    vacant = jax.random.randint(jax.random.fold_in(key, 31), (SEGS,), 0, 8, dtype=jnp.int32) == 0
    forced = jax.random.randint(jax.random.fold_in(key, 37), (), 0, SEGS, dtype=jnp.int32)
    vacant = vacant | (jnp.arange(SEGS, dtype=jnp.int32) == forced)
    dom_ids = jnp.arange(dom_count, dtype=jnp.int32)
    window_ids = ((dom_ids[:, None] * SEG_DEV + jnp.arange(window_len, dtype=jnp.int32)[None, :]) % SEGS).astype(jnp.int32)
    blocked = vacant[window_ids].astype(jnp.int32)
    order = jnp.argsort(blocked, axis=1, stable=True).astype(jnp.int32)
    allowed = jnp.maximum(window_len - jnp.sum(blocked, axis=1), 1).astype(jnp.int32)
    row_dom = (jnp.arange(ROWS, dtype=jnp.int32) // (ROWS_DEV * N_REP)).astype(jnp.int32)
    raw_pick = jax.random.randint(jax.random.fold_in(key, 41), (ROWS,), 0, 1 << 24, dtype=jnp.int32)
    pick = (raw_pick % allowed[row_dom]).astype(jnp.int32)
    return order[row_dom, pick].astype(jnp.int32)


def set_ends(drawn, own_key, least, top_value):
    longest = drawn.shape.index(max(drawn.shape))
    spots = []
    for shift in (0, 1):
        where = [jax.random.randint(jax.random.fold_in(own_key, axis), (), 0, length) for axis, length in enumerate(drawn.shape)]
        where[longest] = (where[longest] + shift) % drawn.shape[longest]
        spots.append(tuple(where))
    return drawn.at[spots[0]].set(least).at[spots[1]].set(top_value)


def levels(stream_key, extent, cuts, least, high):
    level, own = 1.0, jax.random.fold_in(stream_key, 6)
    for dim, shards_of in cuts:
        steps = jnp.exp(jax.random.uniform(jax.random.fold_in(own, dim), (shards_of,), jnp.float32, least / len(cuts), high / len(cuts)))
        level = level * jnp.repeat(steps, extent[dim] // shards_of).reshape([-1 if axis == dim else 1 for axis in range(len(extent))])
    return level


def centred(key, extent, scale, most, pieces=(), held_as=jnp.bfloat16):
    result = scale * jax.random.normal(key, extent, jnp.float32)
    if pieces:
        result = result * levels(key, extent, pieces, -0.22, 0.18)
    return jnp.clip(result, -most, most).astype(held_as)


def setup_inputs(seed: int = 0) -> dict:
    key_of = jax.random.split(jax.random.key(seed), 12)
    return {
        "ns_shape": centred(key_of[0], (K, P_SIZE), K ** -0.5, 0.75),
        "nm_shape": centred(key_of[1], (K, P_SIZE), K ** -0.5, 0.75),
        "sec_disp": centred(key_of[2], (K, ROWS), 1.0, 6.0, ((1, 32),)),
        "mst_disp": centred(key_of[3], (K, ROWS), 1.0, 6.0, ((1, 32),)),
        "gap_offset": centred(key_of[4], (ROWS,), 1.0, 6.0, ((0, 32),), jnp.float32),
        "quad_weight": jnp.clip(jnp.exp(jax.random.uniform(key_of[5], (P_SIZE,), jnp.float32, math.log(0.25), math.log(4.0))), 0.25, 4.0),
        "jacobian": jnp.clip(jnp.exp(math.log(0.005) - 2.30258502 * jax.random.uniform(key_of[6], (ROWS,), jnp.float32) ** levels(key_of[6], (ROWS,), ((0, 32),), -0.2, 0.2)), 0.0005, 0.005),
        "segment_slot": draw_segment_slot(jax.random.fold_in(key_of[11], 71), 0),
        "face_id": set_ends(jax.random.randint(key_of[8], (ROWS,), 0, 1073741824), jax.random.fold_in(key_of[8], 1), 0, 1073741823).astype(jnp.int32),
        "search_rank": set_ends(jax.random.randint(key_of[9], (ROWS,), 0, 4), jax.random.fold_in(key_of[9], 1), 0, 3).astype(jnp.int32),
        "live_rows": draw_live_rows(jax.random.fold_in(key_of[11], 71), 0),
    }


PENALTY = 400.0
LOWEST_FILL = -1.0e30
FACE_LIMIT = 1073741824


def project(shape_table, displace):
    return lax.dot_general(shape_table, displace, (((0,), (0,)), ((), ())), preferred_element_type=jnp.float32)


def window_stats(gap_field, jac_row, weights, slots, faces, ranks, live, window_len):
    row_pen = jnp.max(-gap_field, axis=0)
    row_gap = jac_row * jnp.dot(weights, gap_field, precision=lax.Precision.HIGHEST)
    row_area = jac_row * jnp.sum(weights)
    penalty_max = jnp.maximum(jax.ops.segment_max(jnp.where(live, row_pen, LOWEST_FILL), slots, num_segments=window_len), LOWEST_FILL)
    best_rank = jnp.maximum(jax.ops.segment_max(jnp.where(live, ranks, -1), slots, num_segments=window_len), -1).astype(jnp.int32)
    chosen = jnp.where(live & (ranks == best_rank[slots]), faces, FACE_LIMIT).astype(jnp.int32)
    lowest_face = jnp.minimum(jax.ops.segment_min(chosen, slots, num_segments=window_len), FACE_LIMIT).astype(jnp.int32)
    gap_sum = jax.ops.segment_sum(jnp.where(live, row_gap, 0.0), slots, num_segments=window_len)
    area_sum = jax.ops.segment_sum(jnp.where(live, row_area, 0.0), slots, num_segments=window_len)
    return penalty_max, best_rank, lowest_face, gap_sum, area_sum


def reference(ns_shape, nm_shape, sec_disp, mst_disp, gap_offset, quad_weight, jacobian, segment_slot, face_id, search_rank, live_rows):
    row_count = ROWS_DEV
    window_len = SEG_DEV + SPILL

    def blocks(values):
        return values.reshape(DEVICES, row_count)

    sec_blocks = sec_disp.reshape(K, DEVICES, row_count).transpose(1, 0, 2)
    mst_blocks = mst_disp.reshape(K, DEVICES, row_count).transpose(1, 0, 2)

    def one_block(block):
        sec_part, mst_part, offset, jac_row, slots, faces, ranks, live_count = block
        gap_field = project(ns_shape, sec_part) - project(nm_shape, mst_part) + offset[None, :]
        live = jnp.arange(row_count, dtype=jnp.int32) < live_count
        load = jnp.where(live[None, :], quad_weight[:, None] * jac_row[None, :] * PENALTY * jnp.maximum(-gap_field, 0.0), 0.0).astype(jnp.bfloat16)
        force = jnp.dot(ns_shape, load, preferred_element_type=jnp.float32).astype(jnp.bfloat16)
        stats = window_stats(gap_field, jac_row, quad_weight, slots, faces, ranks, live, window_len)
        return (force,) + stats

    outputs = lax.map(one_block, (sec_blocks, mst_blocks, blocks(gap_offset), blocks(jacobian), blocks(segment_slot), blocks(face_id), blocks(search_rank), live_rows))
    force_blocks, penalty_max, best_rank, lowest_face, gap_sum, area_sum = outputs
    contact_force = force_blocks.transpose(1, 0, 2).reshape(K, DEVICES * row_count)
    dom_index = (jnp.arange(DEVICES, dtype=jnp.int32) // N_REP).astype(jnp.int32)
    seg_ids = ((dom_index[:, None] * SEG_DEV + jnp.arange(window_len, dtype=jnp.int32)[None, :]) % SEGS).astype(jnp.int32).reshape(-1)
    seg_max = jnp.maximum(jax.ops.segment_max(penalty_max.reshape(-1), seg_ids, num_segments=SEGS), LOWEST_FILL)
    seg_rank = jnp.maximum(jax.ops.segment_max(best_rank.reshape(-1), seg_ids, num_segments=SEGS), -1).astype(jnp.int32)
    chosen = jnp.where(best_rank.reshape(-1) == seg_rank[seg_ids], lowest_face.reshape(-1), FACE_LIMIT).astype(jnp.int32)
    seg_low = jnp.minimum(jax.ops.segment_min(chosen, seg_ids, num_segments=SEGS), FACE_LIMIT).astype(jnp.int32)
    seg_pen = jnp.where(seg_rank < 0, jnp.float32(0.0), seg_max)
    seg_face = jnp.where(seg_rank < 0, -1, seg_low).astype(jnp.int32)
    seg_gap = jax.ops.segment_sum(gap_sum.reshape(-1), seg_ids, num_segments=SEGS)
    mean_gap = jnp.sum(gap_sum) / jnp.sum(area_sum)
    return contact_force, seg_pen, seg_face, seg_gap, mean_gap
```

```python
import functools

import jax
import jax.numpy as jnp
from jax import lax
from jax.experimental import pallas as pl
from jax.experimental.pallas import tpu as pltpu
from jax.sharding import PartitionSpec as P

SEG_DEV = 1024
SPILL = 256
LANES = 128
SUB = 8
GROUPS = (SEG_DEV + SPILL) // LANES
OWN_GROUPS = SEG_DEV // LANES
PAD_GROUPS = 16

PENALTY = 400.0
LOWEST_FILL = -1e30
FACE_LIMIT = 1073741824
FACE_MASK = FACE_LIMIT - 1
KEY_LOW = -2147483648
MESH = pl.DeviceIdType.MESH
TILE = 256


def split3(x):
    a = x.astype(jnp.bfloat16)
    rest = x - a.astype(jnp.float32)
    b = rest.astype(jnp.bfloat16)
    c = (rest - b.astype(jnp.float32)).astype(jnp.bfloat16)
    return a, b, c


def dense_kernel(
    live_ref, ns_ref, nm_ref, qw_ref, sec_ref, mst_ref, off_ref, jac_ref, slot_ref,
    force_ref, pen_ref, seg_ref,
    wt_ref, qcol_ref, qsum_ref,
):
    step = pl.program_id(0)
    k_size, p_size = ns_ref.shape
    rows = sec_ref.shape[1]
    lines = rows // LANES
    per_tile = TILE // LANES

    @pl.when(step == 0)
    def _():
        w = jnp.concatenate([ns_ref[...], -nm_ref[...]], axis=0).astype(jnp.float32)
        qrow = qw_ref[...]
        wt = w.T
        wt_ref[0:p_size, :] = wt.astype(jnp.bfloat16)
        qmat = jnp.broadcast_to(qrow, (LANES, p_size)).T
        qcol_ref[...] = qmat
        v = jnp.sum(wt * qmat, axis=0, keepdims=True)
        a, b, c = split3(v)
        pick = lax.broadcasted_iota(jnp.int32, (16, 2 * k_size), 0)
        stacked = jnp.where(
            pick == 0,
            a.astype(jnp.float32),
            jnp.where(pick == 1, b.astype(jnp.float32), jnp.where(pick == 2, c.astype(jnp.float32), 0.0)),
        )
        wt_ref[p_size:, :] = stacked.astype(jnp.bfloat16)
        qsum_ref[...] = jnp.broadcast_to(jnp.sum(qmat, axis=0, keepdims=True), (SUB, LANES))
        seg_ref[...] = jnp.zeros_like(seg_ref)

    live_count = live_ref[0]
    first = step * rows
    qcol = qcol_ref[...]
    qsum = qsum_ref[0:1, :]
    wt = wt_ref[...]
    ns = ns_ref[...]
    lane = lax.broadcasted_iota(jnp.int32, (1, LANES), 1)
    seg_total = jnp.zeros((PAD_GROUPS, LANES), jnp.float32)
    for tile in range(rows // TILE):
        cols = pl.ds(tile * TILE, TILE)
        x = jnp.concatenate([sec_ref[:, cols], mst_ref[:, cols]], axis=0)
        field = jnp.dot(wt, x, preferred_element_type=jnp.float32)
        pieces = []
        scales = []
        for part in range(per_tile):
            line = tile * per_tile + part
            here = slice(part * LANES, (part + 1) * LANES)
            offset = off_ref[line : line + 1, :]
            live = (lane + (first + line * LANES)) < live_count
            jac = jac_ref[line : line + 1, :]
            jac_live = jnp.where(live, jac, 0.0)
            gap = field[:p_size, here] + offset
            lowest = jnp.min(gap, axis=0, keepdims=True)
            pen_ref[line : line + 1, :] = jnp.where(live, -lowest, LOWEST_FILL)
            pieces.append((qcol * jnp.maximum(-gap, 0.0)).astype(jnp.bfloat16))
            scales.append(jac_live * PENALTY)
            summed = jnp.sum(field[p_size : p_size + SUB, here], axis=0, keepdims=True)
            row_gap = jac_live * (summed + offset * qsum)
            slot = slot_ref[line : line + 1, :]
            hi = slot >> 7
            lo = slot & (LANES - 1)
            hit_hi = lax.broadcasted_iota(jnp.int32, (PAD_GROUPS, LANES), 0) == hi
            hit_lo = lax.broadcasted_iota(jnp.int32, (LANES, LANES), 0) == lo
            spread = jnp.where(hit_hi, row_gap, 0.0)
            a, b, c = split3(spread)
            left = jnp.concatenate([a, b, c], axis=0)
            right = jnp.where(hit_lo, 1.0, 0.0).astype(jnp.bfloat16)
            got = lax.dot_general(
                left, right, (((1,), (1,)), ((), ())), preferred_element_type=jnp.float32
            )
            seg_total = seg_total + (
                got[0:PAD_GROUPS] + got[PAD_GROUPS : 2 * PAD_GROUPS] + got[2 * PAD_GROUPS :]
            )
        load = jnp.concatenate(pieces, axis=1)
        force = jnp.dot(ns, load, preferred_element_type=jnp.float32)
        force_ref[:, cols] = (force * jnp.concatenate(scales, axis=1)).astype(jnp.bfloat16)
    seg_ref[...] += seg_total


def merge_kernel(
    n_dom, n_rep,
    live_ref, qw_ref, slot_ref, face_ref, rank_ref, pen_ref, jac_ref, seg_ref,
    out_pen, out_face, out_gap, out_mean,
    pen_g, key_g, acc_pen, acc_key,
    sp_f, sp_i, ow_f, ow_i, tot_d, tot_r, tot_s,
    spill_f, spill_i, spill_t, own_f, own_i, own_t,
    s_spf, r_spf, s_spi, r_spi, s_owf, r_owf, s_owi, r_owi, s_td, r_td, s_tr, r_tr,
):
    dom = lax.axis_index("dom")
    rep = lax.axis_index("rep")
    lines = slot_ref.shape[0]

    def dev(d, r):
        return {"dom": lax.rem(d + n_dom, n_dom), "rep": lax.rem(r + n_rep, n_rep)}

    barrier = pltpu.get_barrier_semaphore()

    def greet(d, r):
        pl.semaphore_signal(barrier, inc=1, device_id=dev(d, r), device_id_type=MESH)

    for j in range(1, n_rep):
        greet(dom, rep + j)
        greet(dom + 1, rep + j)
        greet(dom - 1, rep + j)

    def greet_dom(j, carry):
        greet(dom + j, rep)
        return carry

    lax.fori_loop(1, n_dom, greet_dom, 0)

    live_count = live_ref[0]
    row_id = (
        lax.broadcasted_iota(jnp.int32, (lines, LANES), 0) * LANES
        + lax.broadcasted_iota(jnp.int32, (lines, LANES), 1)
    )
    live = row_id < live_count
    slot = slot_ref[...]
    hi = slot >> 7
    key = jnp.where(
        live, ((rank_ref[...] - 2) << 30) + (FACE_MASK - face_ref[...]), KEY_LOW
    )
    pen = pen_ref[...]
    for g in range(GROUPS):
        inside = hi == g
        pen_g[g * lines : (g + 1) * lines, :] = jnp.where(inside, pen, LOWEST_FILL)
        key_g[g * lines : (g + 1) * lines, :] = jnp.where(inside, key, KEY_LOW)

    total_gap = jnp.sum(jnp.sum(seg_ref[...], axis=0, keepdims=True), axis=1, keepdims=True)
    area_rows = jnp.where(live, jac_ref[...], 0.0)
    total_area = jnp.sum(
        jnp.sum(area_rows, axis=0, keepdims=True), axis=1, keepdims=True
    ) * jnp.sum(qw_ref[...], axis=1, keepdims=True)
    sub = lax.broadcasted_iota(jnp.int32, (SUB, LANES), 0)
    pair = jnp.where(sub == 0, total_gap, jnp.where(sub == 1, total_area, 0.0))
    tot_s[...] = pair
    tot_d[dom] = pair

    pl.semaphore_wait(barrier, 3 * (n_rep - 1) + n_dom - 1)

    def tot_dom(j):
        return pltpu.make_async_remote_copy(
            src_ref=tot_s, dst_ref=tot_d.at[dom],
            send_sem=s_td.at[j], recv_sem=r_td.at[dom],
            device_id=dev(dom + j, rep), device_id_type=MESH,
        )

    def tot_dom_in(j):
        source = lax.rem(dom - j + n_dom, n_dom)
        return pltpu.make_async_remote_copy(
            src_ref=tot_s, dst_ref=tot_d.at[source],
            send_sem=s_td.at[j], recv_sem=r_td.at[source],
            device_id=dev(dom + j, rep), device_id_type=MESH,
        )

    def start_tot(j, carry):
        tot_dom(j).start()
        return carry

    lax.fori_loop(1, n_dom, start_tot, 0)

    def scan_groups(g0, g1, per):
        count = g1 - g0
        width = SUB * per

        def one(block, carry):
            base = block * width
            marks = [
                lax.broadcasted_iota(jnp.int32, (SUB, LANES), 0) + (base + SUB * q)
                for q in range(per)
            ]

            def body(i, accs):
                accs = list(accs)
                c = i
                lo = slot_ref[pl.ds(c, SUB, stride=0), :] & (LANES - 1)
                hits = [lo == m for m in marks]
                for g in range(count):
                    at = (g0 + g) * lines + c
                    pv = pen_g[pl.ds(at, SUB, stride=0), :]
                    kv = key_g[pl.ds(at, SUB, stride=0), :]
                    for q in range(per):
                        n = 2 * (g * per + q)
                        accs[n] = jnp.maximum(accs[n], jnp.where(hits[q], pv, LOWEST_FILL))
                        accs[n + 1] = jnp.maximum(accs[n + 1], jnp.where(hits[q], kv, KEY_LOW))
                return tuple(accs)

            start = (
                jnp.full((SUB, LANES), LOWEST_FILL, jnp.float32),
                jnp.full((SUB, LANES), KEY_LOW, jnp.int32),
            ) * (count * per)
            accs = lax.fori_loop(0, lines, body, start, unroll=4)
            for g in range(count):
                for q in range(per):
                    n = 2 * (g * per + q)
                    rows = pl.ds((g0 + g) * LANES + base + SUB * q, SUB)
                    acc_pen[rows, :] = accs[n]
                    acc_key[rows, :] = accs[n + 1]
            return carry

        lax.fori_loop(0, LANES // width, one, 0)

    def gather_group(g):
        rows = pl.ds(g * LANES, LANES)
        top = jnp.max(acc_pen[rows, :].T, axis=0, keepdims=True)
        best = jnp.max(acc_key[rows, :].T, axis=0, keepdims=True)
        return top, best

    def decode(top, best):
        none = top < LOWEST_FILL * 0.5
        rank = jnp.where(none, -1, (best >> 30) + 2)
        face = jnp.where(none, FACE_LIMIT, FACE_MASK - (best & FACE_MASK))
        return rank, face

    scan_groups(OWN_GROUPS, GROUPS, 4)
    spill_f[0] = jnp.full((SUB, LANES), LOWEST_FILL, jnp.float32)
    spill_i[0] = jnp.full((SUB, LANES), -1, jnp.int32)
    spill_i[1] = jnp.full((SUB, LANES), FACE_LIMIT, jnp.int32)
    spill_f[1] = seg_ref[OWN_GROUPS:, :]
    for g in range(OWN_GROUPS, GROUPS):
        top, best = gather_group(g)
        rank, face = decode(top, best)
        at = pl.ds(g - OWN_GROUPS, 1)
        spill_f[0, at, :] = top
        spill_i[0, at, :] = rank
        spill_i[1, at, :] = face

    def spill_copy(j, source):
        return (
            pltpu.make_async_remote_copy(
                src_ref=spill_f, dst_ref=sp_f.at[source],
                send_sem=s_spf.at[j], recv_sem=r_spf.at[source],
                device_id=dev(dom + 1, rep + j), device_id_type=MESH,
            ),
            pltpu.make_async_remote_copy(
                src_ref=spill_i, dst_ref=sp_i.at[source],
                send_sem=s_spi.at[j], recv_sem=r_spi.at[source],
                device_id=dev(dom + 1, rep + j), device_id_type=MESH,
            ),
        )

    for j in range(n_rep):
        for copy in spill_copy(j, rep):
            copy.start()

    def wait_tot(j, carry):
        tot_dom_in(j).wait_recv()
        return carry

    lax.fori_loop(1, n_dom, wait_tot, 0)

    def add_tot(j, total):
        return total + tot_d[j]

    dom_total = lax.fori_loop(0, n_dom, add_tot, jnp.zeros((SUB, LANES), jnp.float32))
    own_t[...] = dom_total
    tot_r[rep] = dom_total

    def rep_tot(j, source):
        return pltpu.make_async_remote_copy(
            src_ref=own_t, dst_ref=tot_r.at[source],
            send_sem=s_tr.at[j], recv_sem=r_tr.at[source],
            device_id=dev(dom, rep + j), device_id_type=MESH,
        )

    for j in range(1, n_rep):
        rep_tot(j, rep).start()

    scan_groups(0, OWN_GROUPS, 2)
    own_f[1] = seg_ref[:OWN_GROUPS, :]
    for g in range(OWN_GROUPS):
        top, best = gather_group(g)
        rank, face = decode(top, best)
        at = pl.ds(g, 1)
        own_f[0, at, :] = top
        own_i[0, at, :] = rank
        own_i[1, at, :] = face

    def own_copy(j, source):
        return (
            pltpu.make_async_remote_copy(
                src_ref=own_f, dst_ref=ow_f.at[source],
                send_sem=s_owf.at[j], recv_sem=r_owf.at[source],
                device_id=dev(dom, rep + j), device_id_type=MESH,
            ),
            pltpu.make_async_remote_copy(
                src_ref=own_i, dst_ref=ow_i.at[source],
                send_sem=s_owi.at[j], recv_sem=r_owi.at[source],
                device_id=dev(dom, rep + j), device_id_type=MESH,
            ),
        )

    for j in range(1, n_rep):
        for copy in own_copy(j, rep):
            copy.start()
    ow_f[rep] = own_f[...]
    ow_i[rep] = own_i[...]

    def encode(rank, face):
        return jnp.where(rank < 0, KEY_LOW, ((rank - 2) << 30) + (FACE_MASK - face))

    for j in range(1, n_rep):
        rep_tot(j, lax.rem(rep - j + n_rep, n_rep)).wait_recv()
    whole = tot_r[0]
    for r in range(1, n_rep):
        whole = whole + tot_r[r]
    out_mean[0] = jnp.sum(whole[0:1, 0:1]) / jnp.sum(whole[1:2, 0:1])

    for j in range(n_rep):
        for copy in spill_copy(j, lax.rem(rep - j + n_rep, n_rep)):
            copy.wait_recv()
    pen_s, gap_s = sp_f[0, 0], sp_f[0, 1]
    key_s = encode(sp_i[0, 0], sp_i[0, 1])
    for r in range(1, n_rep):
        pen_s = jnp.maximum(pen_s, sp_f[r, 0])
        gap_s = gap_s + sp_f[r, 1]
        key_s = jnp.maximum(key_s, encode(sp_i[r, 0], sp_i[r, 1]))
    for j in range(1, n_rep):
        for copy in own_copy(j, lax.rem(rep - j + n_rep, n_rep)):
            copy.wait_recv()
    pen_o, key_o, gap_o = pen_s, key_s, ow_f[0, 1]
    for r in range(n_rep):
        pen_o = jnp.maximum(pen_o, ow_f[r, 0])
        key_o = jnp.maximum(key_o, encode(ow_i[r, 0], ow_i[r, 1]))
        if r:
            gap_o = gap_o + ow_f[r, 1]
    none = pen_o < LOWEST_FILL * 0.5
    out_pen[...] = jnp.where(none, 0.0, pen_o)
    out_face[...] = jnp.where(none, -1, FACE_MASK - (key_o & FACE_MASK))
    out_gap[...] = gap_o + gap_s

    def end_tot(j, carry):
        tot_dom(j).wait_send()
        return carry

    lax.fori_loop(1, n_dom, end_tot, 0)
    for j in range(1, n_rep):
        rep_tot(j, rep).wait_send()
        for copy in own_copy(j, rep):
            copy.wait_send()
    for j in range(n_rep):
        for copy in spill_copy(j, rep):
            copy.wait_send()


def solution(mesh):
    n_dom, n_rep = mesh.shape["dom"], mesh.shape["rep"]

    def shards(ns, nm, sec, mst, off, qw, jac, slot, face, rank, live):
        k_size, p_size = ns.shape
        rows = sec.shape[1]
        lines = rows // LANES
        block = 1024
        b_lines = block // LANES
        grid = rows // block

        def lined(x):
            return x.reshape(lines, LANES)

        qrow = qw.reshape(1, p_size)
        off, jac, slot, face, rank = (lined(x) for x in (off, jac, slot, face, rank))
        smem = pl.BlockSpec(memory_space=pltpu.SMEM)
        full = lambda shape: pl.BlockSpec(shape, lambda i: (0, 0))
        line_spec = pl.BlockSpec((b_lines, LANES), lambda i: (i, 0))
        wide = pl.BlockSpec((k_size, block), lambda i: (0, i))
        force, pen, seg = pl.pallas_call(
            dense_kernel,
            grid=(grid,),
            out_shape=(
                jax.ShapeDtypeStruct((k_size, rows), jnp.bfloat16),
                jax.ShapeDtypeStruct((lines, LANES), jnp.float32),
                jax.ShapeDtypeStruct((PAD_GROUPS, LANES), jnp.float32),
            ),
            in_specs=[
                smem, full((k_size, p_size)), full((k_size, p_size)), full((1, p_size)),
                wide, wide, line_spec, line_spec, line_spec,
            ],
            out_specs=(wide, line_spec, full((PAD_GROUPS, LANES))),
            scratch_shapes=[
                pltpu.VMEM((p_size + 16, 2 * k_size), jnp.bfloat16),
                pltpu.VMEM((p_size, LANES), jnp.float32),
                pltpu.VMEM((SUB, LANES), jnp.float32),
            ],
            compiler_params=pltpu.CompilerParams(dimension_semantics=("arbitrary",)),
        )(live, ns, nm, qrow, sec, mst, off, jac, slot)

        vmem = pl.BlockSpec(memory_space=pltpu.VMEM)
        tile_f = (2, SUB, LANES)
        sems = pltpu.SemaphoreType.DMA
        seg_pen, seg_face, seg_gap, mean = pl.pallas_call(
            functools.partial(merge_kernel, n_dom, n_rep),
            out_shape=(
                jax.ShapeDtypeStruct((SUB, LANES), jnp.float32),
                jax.ShapeDtypeStruct((SUB, LANES), jnp.int32),
                jax.ShapeDtypeStruct((SUB, LANES), jnp.float32),
                jax.ShapeDtypeStruct((1,), jnp.float32),
            ),
            in_specs=[smem] + [vmem] * 7,
            out_specs=(vmem, vmem, vmem, smem),
            scratch_shapes=[
                pltpu.VMEM((GROUPS * lines + SUB, LANES), jnp.float32),
                pltpu.VMEM((GROUPS * lines + SUB, LANES), jnp.int32),
                pltpu.VMEM((GROUPS * LANES, LANES), jnp.float32),
                pltpu.VMEM((GROUPS * LANES, LANES), jnp.int32),
                pltpu.VMEM((n_rep,) + tile_f, jnp.float32),
                pltpu.VMEM((n_rep,) + tile_f, jnp.int32),
                pltpu.VMEM((n_rep,) + tile_f, jnp.float32),
                pltpu.VMEM((n_rep,) + tile_f, jnp.int32),
                pltpu.VMEM((n_dom, SUB, LANES), jnp.float32),
                pltpu.VMEM((n_rep, SUB, LANES), jnp.float32),
                pltpu.VMEM((SUB, LANES), jnp.float32),
                pltpu.VMEM(tile_f, jnp.float32),
                pltpu.VMEM(tile_f, jnp.int32),
                pltpu.VMEM((SUB, LANES), jnp.float32),
                pltpu.VMEM(tile_f, jnp.float32),
                pltpu.VMEM(tile_f, jnp.int32),
                pltpu.VMEM((SUB, LANES), jnp.float32),
                sems((n_rep,)), sems((n_rep,)), sems((n_rep,)), sems((n_rep,)),
                sems((n_rep,)), sems((n_rep,)), sems((n_rep,)), sems((n_rep,)),
                sems((n_dom,)), sems((n_dom,)), sems((n_rep,)), sems((n_rep,)),
            ],
            compiler_params=pltpu.CompilerParams(collective_id=0, has_side_effects=True),
        )(live, qrow, slot, face, rank, pen, jac, seg)
        return (
            force,
            seg_pen.reshape(SEG_DEV),
            seg_face.reshape(SEG_DEV),
            seg_gap.reshape(SEG_DEV),
            mean.reshape(()),
        )

    return jax.shard_map(
        shards,
        mesh=mesh,
        in_specs=(
            P(),
            P(),
            P(None, ("dom", "rep")),
            P(None, ("dom", "rep")),
            P(("dom", "rep")),
            P(),
            P(("dom", "rep")),
            P(("dom", "rep")),
            P(("dom", "rep")),
            P(("dom", "rep")),
            P(("dom", "rep")),
        ),
        out_specs=(P(None, ("dom", "rep")), P("dom"), P("dom"), P("dom"), P()),
        check_vma=False,
    )
```

```python
import functools

import jax
import jax.numpy as jnp
from jax import lax
from jax.experimental import pallas as pl
from jax.experimental.pallas import tpu as pltpu
from jax.sharding import PartitionSpec as P

SEG_DEV = 1024
SPILL = 256
LANES = 128
SUB = 8
GROUPS = (SEG_DEV + SPILL) // LANES
OWN_GROUPS = SEG_DEV // LANES
PAD_GROUPS = 16

PENALTY = 400.0
LOWEST_FILL = -1e30
FACE_LIMIT = 1073741824
FACE_MASK = FACE_LIMIT - 1
KEY_LOW = -2147483648
MESH = pl.DeviceIdType.MESH
TILE = 256
DEPTH = 16


def split3(x):
    a = x.astype(jnp.bfloat16)
    rest = x - a.astype(jnp.float32)
    b = rest.astype(jnp.bfloat16)
    c = (rest - b.astype(jnp.float32)).astype(jnp.bfloat16)
    return a, b, c


def scan_group(g, depth0, code_ref, slot_ref, pen_ref, key_ref, packs, accs_pen, accs_key):
    all_lines = code_ref.shape[0]
    lane_lo, lane_pen, lane_key = packs
    blocks = DEPTH // SUB
    sub = lax.broadcasted_iota(jnp.int32, (SUB, LANES), 0)
    wants = [(sub + (depth0 + SUB * b)) * PAD_GROUPS + g for b in range(blocks)]

    def pull(i, carry):
        los, pens, keys = (list(part) for part in carry)
        code = code_ref[pl.ds(i, SUB, stride=0), :]
        slot = slot_ref[pl.ds(i, SUB, stride=0), :]
        pen = pen_ref[pl.ds(i, SUB, stride=0), :]
        key = key_ref[pl.ds(i, SUB, stride=0), :]
        for b in range(blocks):
            hit = code == wants[b]
            los[b] = jnp.where(hit, slot, los[b])
            pens[b] = jnp.where(hit, pen, pens[b])
            keys[b] = jnp.where(hit, key, keys[b])
        return tuple(los), tuple(pens), tuple(keys)

    none = jnp.full((SUB, LANES), -1, jnp.int32)
    empty = jnp.full((SUB, LANES), LOWEST_FILL, jnp.float32)
    start = ((none,) * blocks, (empty,) * blocks, (none,) * blocks)
    los, pens, keys = lax.fori_loop(0, all_lines, pull, start, unroll=8)
    for b in range(blocks):
        rows = slice(SUB * b, SUB * (b + 1))
        lane_lo[rows, :] = los[b]
        lane_pen[rows, :] = pens[b]
        lane_key[rows, :] = keys[b]

    tiles = LANES // SUB
    half = tiles // 2
    for part in range(2):
        marks = [sub + (g * LANES + SUB * (part * half + q)) for q in range(half)]
        best_pen = [empty] * half
        best_key = [jnp.full((SUB, LANES), KEY_LOW, jnp.int32)] * half
        for j in range(DEPTH):
            lo = lane_lo[pl.ds(j, SUB, stride=0), :]
            pen = lane_pen[pl.ds(j, SUB, stride=0), :]
            key = lane_key[pl.ds(j, SUB, stride=0), :]
            for q in range(half):
                hit = lo == marks[q]
                best_pen[q] = jnp.maximum(best_pen[q], jnp.where(hit, pen, LOWEST_FILL))
                best_key[q] = jnp.maximum(best_key[q], jnp.where(hit, key, KEY_LOW))
        for q in range(half):
            rows = slice(SUB * (part * half + q), SUB * (part * half + q + 1))
            accs_pen[rows, :] = best_pen[q]
            accs_key[rows, :] = best_key[q]
    top = jnp.max(accs_pen[...].T, axis=0, keepdims=True)
    best = jnp.max(accs_key[...].T, axis=0, keepdims=True)
    return top, best


def dense_kernel(
    live_ref, ns_ref, nm_ref, qw_ref, sec_ref, mst_ref, off_ref, jac_ref, slot_ref,
    face_ref, rank_ref,
    force_ref, pen_ref, seg_ref, code_ref, key_ref, over_pen, over_key,
    wt_ref, qcol_ref, qsum_ref, packs, accs_pen, accs_key,
):
    step = pl.program_id(0)
    all_lines = slot_ref.shape[0]
    k_size, p_size = ns_ref.shape
    rows = sec_ref.shape[1]
    lines = rows // LANES
    per_tile = TILE // LANES

    @pl.when(step == 0)
    def _():
        w = jnp.concatenate([ns_ref[...], -nm_ref[...]], axis=0).astype(jnp.float32)
        qrow = qw_ref[...]
        wt = w.T
        wt_ref[0:p_size, :] = wt.astype(jnp.bfloat16)
        qmat = jnp.broadcast_to(qrow, (LANES, p_size)).T
        qcol_ref[...] = qmat
        v = jnp.sum(wt * qmat, axis=0, keepdims=True)
        a, b, c = split3(v)
        pick = lax.broadcasted_iota(jnp.int32, (16, 2 * k_size), 0)
        stacked = jnp.where(
            pick == 0,
            a.astype(jnp.float32),
            jnp.where(pick == 1, b.astype(jnp.float32), jnp.where(pick == 2, c.astype(jnp.float32), 0.0)),
        )
        wt_ref[p_size:, :] = stacked.astype(jnp.bfloat16)
        qsum_ref[...] = jnp.broadcast_to(jnp.sum(qmat, axis=0, keepdims=True), (SUB, LANES))
        seg_ref[...] = jnp.zeros_like(seg_ref)
        over_pen[...] = jnp.full(over_pen.shape, LOWEST_FILL, jnp.float32)
        over_key[...] = jnp.full(over_key.shape, KEY_LOW, jnp.int32)
        row_id = (
            lax.broadcasted_iota(jnp.int32, (all_lines, LANES), 0) * LANES
            + lax.broadcasted_iota(jnp.int32, (all_lines, LANES), 1)
        )
        alive = row_id < live_ref[0]
        key_ref[...] = ((rank_ref[...] - 2) << 30) + (FACE_MASK - face_ref[...])
        group = jnp.where(alive, slot_ref[...] >> 7, -1)
        before = (
            lax.broadcasted_iota(jnp.int32, (all_lines, all_lines), 1)
            < lax.broadcasted_iota(jnp.int32, (all_lines, all_lines), 0)
        )
        before = jnp.where(before, 1.0, 0.0).astype(jnp.bfloat16)
        code = jnp.full((all_lines, LANES), -1, jnp.int32)
        for g in range(GROUPS):
            mine = group == g
            place = jnp.dot(
                before, jnp.where(mine, 1.0, 0.0).astype(jnp.bfloat16),
                preferred_element_type=jnp.float32,
            ).astype(jnp.int32)
            code = jnp.where(mine, place * PAD_GROUPS + g, code)
        code_ref[...] = code

    live_count = live_ref[0]
    first = step * rows
    line0 = step * lines
    qcol = qcol_ref[...]
    qsum = qsum_ref[0:1, :]
    wt = wt_ref[...]
    ns = ns_ref[...]
    lane = lax.broadcasted_iota(jnp.int32, (1, LANES), 1)
    seg_total = jnp.zeros((PAD_GROUPS, LANES), jnp.float32)
    for tile in range(rows // TILE):
        cols = pl.ds(tile * TILE, TILE)
        x = jnp.concatenate([sec_ref[:, cols], mst_ref[:, cols]], axis=0)
        field = jnp.dot(wt, x, preferred_element_type=jnp.float32)
        pieces = []
        scales = []
        for part in range(per_tile):
            line = tile * per_tile + part
            here = slice(part * LANES, (part + 1) * LANES)
            offset = off_ref[line : line + 1, :]
            live = (lane + (first + line * LANES)) < live_count
            jac = jac_ref[line : line + 1, :]
            jac_live = jnp.where(live, jac, 0.0)
            gap = field[:p_size, here] + offset
            lowest = jnp.min(gap, axis=0, keepdims=True)
            pen_ref[pl.ds(line0 + line, 1), :] = jnp.where(live, -lowest, LOWEST_FILL)
            pieces.append((qcol * jnp.maximum(-gap, 0.0)).astype(jnp.bfloat16))
            scales.append(jac_live * PENALTY)
            summed = jnp.sum(field[p_size : p_size + SUB, here], axis=0, keepdims=True)
            row_gap = jac_live * (summed + offset * qsum)
            slot = slot_ref[pl.ds(line0 + line, 1), :]
            hi = slot >> 7
            lo = slot & (LANES - 1)
            hit_hi = lax.broadcasted_iota(jnp.int32, (PAD_GROUPS, LANES), 0) == hi
            hit_lo = lax.broadcasted_iota(jnp.int32, (LANES, LANES), 0) == lo
            spread = jnp.where(hit_hi, row_gap, 0.0)
            a, b, c = split3(spread)
            left = jnp.concatenate([a, b, c], axis=0)
            right = jnp.where(hit_lo, 1.0, 0.0).astype(jnp.bfloat16)
            got = lax.dot_general(
                left, right, (((1,), (1,)), ((), ())), preferred_element_type=jnp.float32
            )
            seg_total = seg_total + (
                got[0:PAD_GROUPS] + got[PAD_GROUPS : 2 * PAD_GROUPS] + got[2 * PAD_GROUPS :]
            )
        load = jnp.concatenate(pieces, axis=1)
        force = jnp.dot(ns, load, preferred_element_type=jnp.float32)
        force_ref[:, cols] = (force * jnp.concatenate(scales, axis=1)).astype(jnp.bfloat16)
    seg_ref[...] += seg_total

    @pl.when(step == pl.num_programs(0) - 1)
    def _():
        code = code_ref[...]

        @pl.when(jnp.max(code) >= DEPTH * PAD_GROUPS)
        def _():
            def one(g, carry):
                for turn in range(1, all_lines // DEPTH):
                    low = turn * DEPTH * PAD_GROUPS
                    here = ((code & (PAD_GROUPS - 1)) == g) & (code >= low)
                    found = jnp.max(jnp.where(here, 1.0, 0.0)) > 0.5

                    @pl.when(found)
                    def _():
                        top, best = scan_group(
                            g, turn * DEPTH, code_ref, slot_ref, pen_ref, key_ref,
                            packs, accs_pen, accs_key,
                        )
                        at = pl.ds(g, 1)
                        over_pen[at, :] = jnp.maximum(over_pen[at, :], top)
                        over_key[at, :] = jnp.maximum(over_key[at, :], best)
                return carry

            lax.fori_loop(0, GROUPS, one, 0)


def merge_kernel(
    n_dom, n_rep,
    live_ref, qw_ref, slot_ref, code_ref, key_ref, pen_ref, jac_ref, seg_ref, over_pen, over_key,
    out_pen, out_key, out_gap, out_mean,
    lane_lo, lane_pen, lane_key, accs_pen, accs_key,
    sp_f, sp_i, ow_f, ow_i, tot_d, tot_r, tot_s,
    spill_f, spill_i, spill_t, own_f, own_i, own_t,
    s_spf, r_spf, s_spi, r_spi, s_owf, r_owf, s_owi, r_owi, s_td, r_td, s_tr, r_tr,
):
    dom = lax.axis_index("dom")
    rep = lax.axis_index("rep")
    lines = slot_ref.shape[0]

    def dev(d, r):
        return {"dom": lax.rem(d + n_dom, n_dom), "rep": lax.rem(r + n_rep, n_rep)}

    barrier = pltpu.get_barrier_semaphore()

    def greet(d, r):
        pl.semaphore_signal(barrier, inc=1, device_id=dev(d, r), device_id_type=MESH)

    for j in range(1, n_rep):
        greet(dom, rep + j)
        greet(dom + 1, rep + j)
        greet(dom - 1, rep + j)

    def greet_dom(j, carry):
        greet(dom + j, rep)
        return carry

    lax.fori_loop(1, n_dom, greet_dom, 0)

    live_count = live_ref[0]
    row_id = (
        lax.broadcasted_iota(jnp.int32, (lines, LANES), 0) * LANES
        + lax.broadcasted_iota(jnp.int32, (lines, LANES), 1)
    )
    live = row_id < live_count
    total_gap = jnp.sum(jnp.sum(seg_ref[...], axis=0, keepdims=True), axis=1, keepdims=True)
    area_rows = jnp.where(live, jac_ref[...], 0.0)
    total_area = jnp.sum(
        jnp.sum(area_rows, axis=0, keepdims=True), axis=1, keepdims=True
    ) * jnp.sum(qw_ref[...], axis=1, keepdims=True)
    sub = lax.broadcasted_iota(jnp.int32, (SUB, LANES), 0)
    pair = jnp.where(sub == 0, total_gap, jnp.where(sub == 1, total_area, 0.0))
    tot_s[...] = pair
    tot_d[dom] = pair

    def tot_dom(j):
        return pltpu.make_async_remote_copy(
            src_ref=tot_s, dst_ref=tot_d.at[dom],
            send_sem=s_td.at[j], recv_sem=r_td.at[dom],
            device_id=dev(dom + j, rep), device_id_type=MESH,
        )

    def tot_dom_in(j):
        source = lax.rem(dom - j + n_dom, n_dom)
        return pltpu.make_async_remote_copy(
            src_ref=tot_s, dst_ref=tot_d.at[source],
            send_sem=s_td.at[j], recv_sem=r_td.at[source],
            device_id=dev(dom + j, rep), device_id_type=MESH,
        )

    def start_tot(j, carry):
        tot_dom(j).start()
        return carry

    def gather_group(g):
        top, best = scan_group(
            g, 0, code_ref, slot_ref, pen_ref, key_ref,
            (lane_lo, lane_pen, lane_key), accs_pen, accs_key,
        )
        at = pl.ds(g, 1)
        return jnp.maximum(top, over_pen[at, :]), jnp.maximum(best, over_key[at, :])

    def decode(top, best):
        none = top < LOWEST_FILL * 0.5
        rank = jnp.where(none, -1, (best >> 30) + 2)
        face = jnp.where(none, FACE_LIMIT, FACE_MASK - (best & FACE_MASK))
        return rank, face

    spill_f[0] = jnp.full((SUB, LANES), LOWEST_FILL, jnp.float32)
    spill_i[0] = jnp.full((SUB, LANES), -1, jnp.int32)
    spill_i[1] = jnp.full((SUB, LANES), FACE_LIMIT, jnp.int32)
    spill_f[1] = seg_ref[OWN_GROUPS:, :]
    def spill_group(g, carry):
        top, best = gather_group(g)
        rank, face = decode(top, best)
        at = pl.ds(g - OWN_GROUPS, 1)
        spill_f[0, at, :] = top
        spill_i[0, at, :] = rank
        spill_i[1, at, :] = face
        return carry

    lax.fori_loop(OWN_GROUPS, GROUPS, spill_group, 0)

    pl.semaphore_wait(barrier, 3 * (n_rep - 1) + n_dom - 1)

    lax.fori_loop(1, n_dom, start_tot, 0)

    def spill_copy(j, source):
        return (
            pltpu.make_async_remote_copy(
                src_ref=spill_f, dst_ref=sp_f.at[source],
                send_sem=s_spf.at[j], recv_sem=r_spf.at[source],
                device_id=dev(dom + 1, rep + j), device_id_type=MESH,
            ),
            pltpu.make_async_remote_copy(
                src_ref=spill_i, dst_ref=sp_i.at[source],
                send_sem=s_spi.at[j], recv_sem=r_spi.at[source],
                device_id=dev(dom + 1, rep + j), device_id_type=MESH,
            ),
        )

    for j in range(n_rep):
        for copy in spill_copy(j, rep):
            copy.start()

    own_f[1] = seg_ref[:OWN_GROUPS, :]

    def own_group(g, carry):
        top, best = gather_group(g)
        rank, face = decode(top, best)
        at = pl.ds(g, 1)
        own_f[0, at, :] = top
        own_i[0, at, :] = rank
        own_i[1, at, :] = face
        return carry

    lax.fori_loop(0, OWN_GROUPS, own_group, 0)

    def own_copy(j, source):
        return (
            pltpu.make_async_remote_copy(
                src_ref=own_f, dst_ref=ow_f.at[source],
                send_sem=s_owf.at[j], recv_sem=r_owf.at[source],
                device_id=dev(dom, rep + j), device_id_type=MESH,
            ),
            pltpu.make_async_remote_copy(
                src_ref=own_i, dst_ref=ow_i.at[source],
                send_sem=s_owi.at[j], recv_sem=r_owi.at[source],
                device_id=dev(dom, rep + j), device_id_type=MESH,
            ),
        )

    for j in range(1, n_rep):
        for copy in own_copy(j, rep):
            copy.start()
    ow_f[rep] = own_f[...]
    ow_i[rep] = own_i[...]

    def wait_tot(j, carry):
        tot_dom_in(j).wait_recv()
        return carry

    lax.fori_loop(1, n_dom, wait_tot, 0)

    def add_tot(j, total):
        return total + tot_d[j]

    dom_total = lax.fori_loop(0, n_dom, add_tot, jnp.zeros((SUB, LANES), jnp.float32))
    own_t[...] = dom_total
    tot_r[rep] = dom_total

    def rep_tot(j, source):
        return pltpu.make_async_remote_copy(
            src_ref=own_t, dst_ref=tot_r.at[source],
            send_sem=s_tr.at[j], recv_sem=r_tr.at[source],
            device_id=dev(dom, rep + j), device_id_type=MESH,
        )

    for j in range(1, n_rep):
        rep_tot(j, rep).start()

    def encode(rank, face):
        return jnp.where(rank < 0, KEY_LOW, ((rank - 2) << 30) + (FACE_MASK - face))

    for j in range(1, n_rep):
        rep_tot(j, lax.rem(rep - j + n_rep, n_rep)).wait_recv()
    whole = tot_r[0]
    for r in range(1, n_rep):
        whole = whole + tot_r[r]
    out_mean[0] = jnp.sum(whole[0:1, 0:1]) / jnp.sum(whole[1:2, 0:1])

    for j in range(n_rep):
        for copy in spill_copy(j, lax.rem(rep - j + n_rep, n_rep)):
            copy.wait_recv()
    pen_s, gap_s = sp_f[0, 0], sp_f[0, 1]
    key_s = encode(sp_i[0, 0], sp_i[0, 1])
    for r in range(1, n_rep):
        pen_s = jnp.maximum(pen_s, sp_f[r, 0])
        gap_s = gap_s + sp_f[r, 1]
        key_s = jnp.maximum(key_s, encode(sp_i[r, 0], sp_i[r, 1]))
    for j in range(1, n_rep):
        for copy in own_copy(j, lax.rem(rep - j + n_rep, n_rep)):
            copy.wait_recv()
    pen_o, key_o, gap_o = pen_s, key_s, ow_f[0, 1]
    for r in range(n_rep):
        pen_o = jnp.maximum(pen_o, ow_f[r, 0])
        key_o = jnp.maximum(key_o, encode(ow_i[r, 0], ow_i[r, 1]))
        if r:
            gap_o = gap_o + ow_f[r, 1]
    out_pen[...] = pen_o
    out_key[...] = key_o
    out_gap[...] = gap_o + gap_s

    def end_tot(j, carry):
        tot_dom(j).wait_send()
        return carry

    lax.fori_loop(1, n_dom, end_tot, 0)
    for j in range(1, n_rep):
        rep_tot(j, rep).wait_send()
        for copy in own_copy(j, rep):
            copy.wait_send()
    for j in range(n_rep):
        for copy in spill_copy(j, rep):
            copy.wait_send()


def solution(mesh):
    n_dom, n_rep = mesh.shape["dom"], mesh.shape["rep"]

    def shards(ns, nm, sec, mst, off, qw, jac, slot, face, rank, live):
        k_size, p_size = ns.shape
        rows = sec.shape[1]
        lines = rows // LANES
        block = 1024
        b_lines = block // LANES
        grid = rows // block

        def lined(x):
            return x.reshape(lines, LANES)

        qrow = qw.reshape(1, p_size)
        off, jac, slot, face, rank = (lined(x) for x in (off, jac, slot, face, rank))
        smem = pl.BlockSpec(memory_space=pltpu.SMEM)
        full = lambda shape: pl.BlockSpec(shape, lambda i: (0, 0))
        line_spec = pl.BlockSpec((b_lines, LANES), lambda i: (i, 0))
        wide = pl.BlockSpec((k_size, block), lambda i: (0, i))
        whole = full((lines, LANES))
        padded = full((PAD_GROUPS, LANES))
        lane_packs = [
            pltpu.VMEM((DEPTH + SUB, LANES), jnp.int32),
            pltpu.VMEM((DEPTH + SUB, LANES), jnp.float32),
            pltpu.VMEM((DEPTH + SUB, LANES), jnp.int32),
        ]
        lane_accs = [
            pltpu.VMEM((LANES, LANES), jnp.float32),
            pltpu.VMEM((LANES, LANES), jnp.int32),
        ]
        force, pen, seg, code, key, over_pen, over_key = pl.pallas_call(
            dense_kernel,
            grid=(grid,),
            out_shape=(
                jax.ShapeDtypeStruct((k_size, rows), jnp.bfloat16),
                jax.ShapeDtypeStruct((lines, LANES), jnp.float32),
                jax.ShapeDtypeStruct((PAD_GROUPS, LANES), jnp.float32),
                jax.ShapeDtypeStruct((lines, LANES), jnp.int32),
                jax.ShapeDtypeStruct((lines, LANES), jnp.int32),
                jax.ShapeDtypeStruct((PAD_GROUPS, LANES), jnp.float32),
                jax.ShapeDtypeStruct((PAD_GROUPS, LANES), jnp.int32),
            ),
            in_specs=[
                smem, full((k_size, p_size)), full((k_size, p_size)), full((1, p_size)),
                wide, wide, line_spec, line_spec, whole, whole, whole,
            ],
            out_specs=(wide, whole, padded, whole, whole, padded, padded),
            scratch_shapes=[
                pltpu.VMEM((p_size + 16, 2 * k_size), jnp.bfloat16),
                pltpu.VMEM((p_size, LANES), jnp.float32),
                pltpu.VMEM((SUB, LANES), jnp.float32),
                lane_packs,
                *lane_accs,
            ],
            compiler_params=pltpu.CompilerParams(dimension_semantics=("arbitrary",)),
        )(live, ns, nm, qrow, sec, mst, off, jac, slot, face, rank)

        vmem = pl.BlockSpec(memory_space=pltpu.VMEM)
        tile_f = (2, SUB, LANES)
        sems = pltpu.SemaphoreType.DMA
        best_pen, best_key, gap_sum, mean = pl.pallas_call(
            functools.partial(merge_kernel, n_dom, n_rep),
            out_shape=(
                jax.ShapeDtypeStruct((SUB, LANES), jnp.float32),
                jax.ShapeDtypeStruct((SUB, LANES), jnp.int32),
                jax.ShapeDtypeStruct((SUB, LANES), jnp.float32),
                jax.ShapeDtypeStruct((1,), jnp.float32),
            ),
            in_specs=[smem] + [vmem] * 9,
            out_specs=(vmem, vmem, vmem, smem),
            scratch_shapes=[
                *lane_packs,
                *lane_accs,
                pltpu.VMEM((n_rep,) + tile_f, jnp.float32),
                pltpu.VMEM((n_rep,) + tile_f, jnp.int32),
                pltpu.VMEM((n_rep,) + tile_f, jnp.float32),
                pltpu.VMEM((n_rep,) + tile_f, jnp.int32),
                pltpu.VMEM((n_dom, SUB, LANES), jnp.float32),
                pltpu.VMEM((n_rep, SUB, LANES), jnp.float32),
                pltpu.VMEM((SUB, LANES), jnp.float32),
                pltpu.VMEM(tile_f, jnp.float32),
                pltpu.VMEM(tile_f, jnp.int32),
                pltpu.VMEM((SUB, LANES), jnp.float32),
                pltpu.VMEM(tile_f, jnp.float32),
                pltpu.VMEM(tile_f, jnp.int32),
                pltpu.VMEM((SUB, LANES), jnp.float32),
                sems((n_rep,)), sems((n_rep,)), sems((n_rep,)), sems((n_rep,)),
                sems((n_rep,)), sems((n_rep,)), sems((n_rep,)), sems((n_rep,)),
                sems((n_dom,)), sems((n_dom,)), sems((n_rep,)), sems((n_rep,)),
            ],
            compiler_params=pltpu.CompilerParams(collective_id=0, has_side_effects=True),
        )(live, qrow, slot, code, key, pen, jac, seg, over_pen, over_key)
        best_pen, best_key, gap_sum = (x.reshape(SEG_DEV) for x in (best_pen, best_key, gap_sum))
        none = best_pen < LOWEST_FILL * 0.5
        seg_pen = jnp.where(none, 0.0, best_pen)
        seg_face = jnp.where(none, -1, FACE_MASK - (best_key & FACE_MASK))
        seg_gap = jnp.where(none, 0.0, gap_sum)
        return force, seg_pen, seg_face, seg_gap, mean.reshape(())

    return jax.shard_map(
        shards,
        mesh=mesh,
        in_specs=(
            P(),
            P(),
            P(None, ("dom", "rep")),
            P(None, ("dom", "rep")),
            P(("dom", "rep")),
            P(),
            P(("dom", "rep")),
            P(("dom", "rep")),
            P(("dom", "rep")),
            P(("dom", "rep")),
            P(("dom", "rep")),
        ),
        out_specs=(P(None, ("dom", "rep")), P("dom"), P("dom"), P("dom"), P()),
        check_vma=False,
    )
```

```python
import functools

import jax
import jax.numpy as jnp
from jax import lax
from jax.experimental import pallas as pl
from jax.experimental.pallas import tpu as pltpu
from jax.sharding import PartitionSpec as P

SEG_DEV = 1024
SPILL = 256
LANES = 128
SUB = 8
GROUPS = (SEG_DEV + SPILL) // LANES
OWN_GROUPS = SEG_DEV // LANES
PAD_GROUPS = 16

PENALTY = 400.0
LOWEST_FILL = -1e30
FACE_LIMIT = 1073741824
FACE_MASK = FACE_LIMIT - 1
KEY_LOW = -2147483648
MESH = pl.DeviceIdType.MESH
TILE = 256
DEPTH = 16
BLOCK = 1024


def split3(x):
    a = x.astype(jnp.bfloat16)
    rest = x - a.astype(jnp.float32)
    b = rest.astype(jnp.bfloat16)
    c = (rest - b.astype(jnp.float32)).astype(jnp.bfloat16)
    return a, b, c


def scan_group(g, depth0, depth, code_ref, slot_ref, pen_ref, key_ref, packs, accs_pen, accs_key):
    all_lines = code_ref.shape[0]
    lane_lo, lane_pen, lane_key = packs
    blocks = depth // SUB
    sub = lax.broadcasted_iota(jnp.int32, (SUB, LANES), 0)
    wants = [(sub + (depth0 + SUB * b)) * PAD_GROUPS + g for b in range(blocks)]

    def pull(i, carry):
        los, pens, keys = (list(part) for part in carry)
        code = code_ref[pl.ds(i, SUB, stride=0), :]
        slot = slot_ref[pl.ds(i, SUB, stride=0), :]
        pen = pen_ref[pl.ds(i, SUB, stride=0), :]
        key = key_ref[pl.ds(i, SUB, stride=0), :]
        for b in range(blocks):
            hit = code == wants[b]
            los[b] = jnp.where(hit, slot, los[b])
            pens[b] = jnp.where(hit, pen, pens[b])
            keys[b] = jnp.where(hit, key, keys[b])
        return tuple(los), tuple(pens), tuple(keys)

    none = jnp.full((SUB, LANES), -1, jnp.int32)
    empty = jnp.full((SUB, LANES), LOWEST_FILL, jnp.float32)
    start = ((none,) * blocks, (empty,) * blocks, (none,) * blocks)
    los, pens, keys = lax.fori_loop(0, all_lines, pull, start, unroll=8)
    for b in range(blocks):
        rows = slice(SUB * b, SUB * (b + 1))
        lane_lo[rows, :] = los[b]
        lane_pen[rows, :] = pens[b]
        lane_key[rows, :] = keys[b]

    tiles = LANES // SUB
    half = tiles // 2
    for part in range(2):
        marks = [sub + (g * LANES + SUB * (part * half + q)) for q in range(half)]
        best_pen = [empty] * half
        best_key = [jnp.full((SUB, LANES), KEY_LOW, jnp.int32)] * half
        for j in range(depth):
            lo = lane_lo[pl.ds(j, SUB, stride=0), :]
            pen = lane_pen[pl.ds(j, SUB, stride=0), :]
            key = lane_key[pl.ds(j, SUB, stride=0), :]
            for q in range(half):
                hit = lo == marks[q]
                best_pen[q] = jnp.maximum(best_pen[q], jnp.where(hit, pen, LOWEST_FILL))
                best_key[q] = jnp.maximum(best_key[q], jnp.where(hit, key, KEY_LOW))
        for q in range(half):
            rows = slice(SUB * (part * half + q), SUB * (part * half + q + 1))
            accs_pen[rows, :] = best_pen[q]
            accs_key[rows, :] = best_key[q]
    top = jnp.max(accs_pen[...].T, axis=0, keepdims=True)
    best = jnp.max(accs_key[...].T, axis=0, keepdims=True)
    return top, best


def dense_kernel(
    live_ref, ns_ref, nm_ref, qw_ref, sec_ref, mst_ref, off_ref, jac_ref, slot_ref,
    face_ref, rank_ref,
    force_ref, pen_ref, seg_ref, code_ref, key_ref, over_pen, over_key,
    wt_ref, qcol_ref, qsum_ref, packs, accs_pen, accs_key,
):
    step = pl.program_id(0)
    all_lines = slot_ref.shape[0]
    k_size, p_size = ns_ref.shape
    rows = sec_ref.shape[1]
    lines = rows // LANES
    per_tile = TILE // LANES

    @pl.when(step == 0)
    def _():
        w = jnp.concatenate([ns_ref[...], -nm_ref[...]], axis=0).astype(jnp.float32)
        qrow = qw_ref[...]
        wt = w.T
        wt_ref[0:p_size, :] = wt.astype(jnp.bfloat16)
        qmat = jnp.broadcast_to(qrow, (LANES, p_size)).T
        qcol_ref[...] = qmat
        v = jnp.sum(wt * qmat, axis=0, keepdims=True)
        a, b, c = split3(v)
        pick = lax.broadcasted_iota(jnp.int32, (16, 2 * k_size), 0)
        stacked = jnp.where(
            pick == 0,
            a.astype(jnp.float32),
            jnp.where(pick == 1, b.astype(jnp.float32), jnp.where(pick == 2, c.astype(jnp.float32), 0.0)),
        )
        wt_ref[p_size:, :] = stacked.astype(jnp.bfloat16)
        qsum_ref[...] = jnp.broadcast_to(jnp.sum(qmat, axis=0, keepdims=True), (SUB, LANES))
        seg_ref[...] = jnp.zeros_like(seg_ref)
        over_pen[...] = jnp.full(over_pen.shape, LOWEST_FILL, jnp.float32)
        over_key[...] = jnp.full(over_key.shape, KEY_LOW, jnp.int32)
        row_id = (
            lax.broadcasted_iota(jnp.int32, (all_lines, LANES), 0) * LANES
            + lax.broadcasted_iota(jnp.int32, (all_lines, LANES), 1)
        )
        alive = row_id < live_ref[0]
        key_ref[...] = ((rank_ref[...] - 2) << 30) + (FACE_MASK - face_ref[...])
        group = jnp.where(alive, slot_ref[...] >> 7, -1)
        before = (
            lax.broadcasted_iota(jnp.int32, (all_lines, all_lines), 1)
            < lax.broadcasted_iota(jnp.int32, (all_lines, all_lines), 0)
        )
        before = jnp.where(before, 1.0, 0.0).astype(jnp.bfloat16)
        code = jnp.full((all_lines, LANES), -1, jnp.int32)
        for g in range(GROUPS):
            mine = group == g
            place = jnp.dot(
                before, jnp.where(mine, 1.0, 0.0).astype(jnp.bfloat16),
                preferred_element_type=jnp.float32,
            ).astype(jnp.int32)
            code = jnp.where(mine, place * PAD_GROUPS + g, code)
        code_ref[...] = code

    live_count = live_ref[0]
    first = step * rows
    line0 = step * lines
    qcol = qcol_ref[...]
    qsum = qsum_ref[0:1, :]
    wt = wt_ref[...]
    ns = ns_ref[...]
    lane = lax.broadcasted_iota(jnp.int32, (1, LANES), 1)
    seg_total = jnp.zeros((PAD_GROUPS, LANES), jnp.float32)
    for tile in range(rows // TILE):
        cols = pl.ds(tile * TILE, TILE)
        x = jnp.concatenate([sec_ref[:, cols], mst_ref[:, cols]], axis=0)
        field = jnp.dot(wt, x, preferred_element_type=jnp.float32)
        pieces = []
        scales = []
        for part in range(per_tile):
            line = tile * per_tile + part
            here = slice(part * LANES, (part + 1) * LANES)
            offset = off_ref[line : line + 1, :]
            live = (lane + (first + line * LANES)) < live_count
            jac = jac_ref[line : line + 1, :]
            jac_live = jnp.where(live, jac, 0.0)
            gap = field[:p_size, here] + offset
            lowest = jnp.min(gap, axis=0, keepdims=True)
            pen_ref[pl.ds(line0 + line, 1), :] = jnp.where(live, -lowest, LOWEST_FILL)
            pieces.append((qcol * jnp.maximum(-gap, 0.0)).astype(jnp.bfloat16))
            scales.append(jac_live * PENALTY)
            summed = jnp.sum(field[p_size : p_size + SUB, here], axis=0, keepdims=True)
            row_gap = jac_live * (summed + offset * qsum)
            slot = slot_ref[pl.ds(line0 + line, 1), :]
            hi = slot >> 7
            lo = slot & (LANES - 1)
            hit_hi = lax.broadcasted_iota(jnp.int32, (PAD_GROUPS, LANES), 0) == hi
            hit_lo = lax.broadcasted_iota(jnp.int32, (LANES, LANES), 0) == lo
            spread = jnp.where(hit_hi, row_gap, 0.0)
            a, b, c = split3(spread)
            left = jnp.concatenate([a, b, c], axis=0)
            right = jnp.where(hit_lo, 1.0, 0.0).astype(jnp.bfloat16)
            got = lax.dot_general(
                left, right, (((1,), (1,)), ((), ())), preferred_element_type=jnp.float32
            )
            seg_total = seg_total + (
                got[0:PAD_GROUPS] + got[PAD_GROUPS : 2 * PAD_GROUPS] + got[2 * PAD_GROUPS :]
            )
        load = jnp.concatenate(pieces, axis=1)
        force = jnp.dot(ns, load, preferred_element_type=jnp.float32)
        force_ref[:, cols] = (force * jnp.concatenate(scales, axis=1)).astype(jnp.bfloat16)
    seg_ref[...] += seg_total

    @pl.when(step == pl.num_programs(0) - 1)
    def _():
        def one(worst):
            code = code_ref[...]
            g = worst & (PAD_GROUPS - 1)
            low = (worst >> 4) & -SUB
            top, best = scan_group(
                g, low, SUB, code_ref, slot_ref, pen_ref, key_ref, packs, accs_pen, accs_key
            )
            at = pl.ds(g, 1)
            over_pen[at, :] = jnp.maximum(over_pen[at, :], top)
            over_key[at, :] = jnp.maximum(over_key[at, :], best)
            done = ((code & (PAD_GROUPS - 1)) == g) & (code >= low * PAD_GROUPS)
            code = jnp.where(done, -1, code)
            code_ref[...] = code
            return jnp.max(code)

        lax.while_loop(lambda worst: worst >= DEPTH * PAD_GROUPS, one, jnp.max(code_ref[...]))


def merge_kernel(
    n_dom, n_rep,
    live_ref, qw_ref, slot_ref, code_ref, key_ref, pen_ref, jac_ref, seg_ref, over_pen, over_key,
    out_pen, out_key, out_gap, out_mean,
    lane_lo, lane_pen, lane_key, accs_pen, accs_key,
    sp_f, sp_i, ow_f, ow_i, tot_d, tot_r, tot_s,
    spill_f, spill_i, spill_t, own_f, own_i, own_t,
    s_spf, r_spf, s_spi, r_spi, s_owf, r_owf, s_owi, r_owi, s_td, r_td, s_tr, r_tr,
):
    dom = lax.axis_index("dom")
    rep = lax.axis_index("rep")
    lines = slot_ref.shape[0]

    def dev(d, r):
        return {"dom": lax.rem(d + n_dom, n_dom), "rep": lax.rem(r + n_rep, n_rep)}

    barrier = pltpu.get_barrier_semaphore()

    def greet(d, r):
        pl.semaphore_signal(barrier, inc=1, device_id=dev(d, r), device_id_type=MESH)

    for j in range(1, n_rep):
        greet(dom, rep + j)
        greet(dom + 1, rep + j)
        greet(dom - 1, rep + j)

    def greet_dom(j, carry):
        greet(dom + j, rep)
        return carry

    lax.fori_loop(1, n_dom, greet_dom, 0)

    live_count = live_ref[0]
    row_id = (
        lax.broadcasted_iota(jnp.int32, (lines, LANES), 0) * LANES
        + lax.broadcasted_iota(jnp.int32, (lines, LANES), 1)
    )
    live = row_id < live_count
    total_gap = jnp.sum(jnp.sum(seg_ref[...], axis=0, keepdims=True), axis=1, keepdims=True)
    area_rows = jnp.where(live, jac_ref[...], 0.0)
    total_area = jnp.sum(
        jnp.sum(area_rows, axis=0, keepdims=True), axis=1, keepdims=True
    ) * jnp.sum(qw_ref[...], axis=1, keepdims=True)
    sub = lax.broadcasted_iota(jnp.int32, (SUB, LANES), 0)
    pair = jnp.where(sub == 0, total_gap, jnp.where(sub == 1, total_area, 0.0))
    tot_s[...] = pair
    tot_d[dom] = pair

    def tot_dom(j):
        return pltpu.make_async_remote_copy(
            src_ref=tot_s, dst_ref=tot_d.at[dom],
            send_sem=s_td.at[j], recv_sem=r_td.at[dom],
            device_id=dev(dom + j, rep), device_id_type=MESH,
        )

    def tot_dom_in(j):
        source = lax.rem(dom - j + n_dom, n_dom)
        return pltpu.make_async_remote_copy(
            src_ref=tot_s, dst_ref=tot_d.at[source],
            send_sem=s_td.at[j], recv_sem=r_td.at[source],
            device_id=dev(dom + j, rep), device_id_type=MESH,
        )

    def start_tot(j, carry):
        tot_dom(j).start()
        return carry

    def gather_group(g):
        top, best = scan_group(
            g, 0, DEPTH, code_ref, slot_ref, pen_ref, key_ref,
            (lane_lo, lane_pen, lane_key), accs_pen, accs_key,
        )
        at = pl.ds(g, 1)
        return jnp.maximum(top, over_pen[at, :]), jnp.maximum(best, over_key[at, :])

    def decode(top, best):
        none = top < LOWEST_FILL * 0.5
        rank = jnp.where(none, -1, (best >> 30) + 2)
        face = jnp.where(none, FACE_LIMIT, FACE_MASK - (best & FACE_MASK))
        return rank, face

    spill_f[0] = jnp.full((SUB, LANES), LOWEST_FILL, jnp.float32)
    spill_i[0] = jnp.full((SUB, LANES), -1, jnp.int32)
    spill_i[1] = jnp.full((SUB, LANES), FACE_LIMIT, jnp.int32)
    spill_f[1] = seg_ref[OWN_GROUPS:, :]
    def spill_group(g, carry):
        top, best = gather_group(g)
        rank, face = decode(top, best)
        at = pl.ds(g - OWN_GROUPS, 1)
        spill_f[0, at, :] = top
        spill_i[0, at, :] = rank
        spill_i[1, at, :] = face
        return carry

    lax.fori_loop(OWN_GROUPS, GROUPS, spill_group, 0)

    pl.semaphore_wait(barrier, 3 * (n_rep - 1) + n_dom - 1)

    lax.fori_loop(1, n_dom, start_tot, 0)

    def spill_copy(j, source):
        return (
            pltpu.make_async_remote_copy(
                src_ref=spill_f, dst_ref=sp_f.at[source],
                send_sem=s_spf.at[j], recv_sem=r_spf.at[source],
                device_id=dev(dom + 1, rep + j), device_id_type=MESH,
            ),
            pltpu.make_async_remote_copy(
                src_ref=spill_i, dst_ref=sp_i.at[source],
                send_sem=s_spi.at[j], recv_sem=r_spi.at[source],
                device_id=dev(dom + 1, rep + j), device_id_type=MESH,
            ),
        )

    for j in range(n_rep):
        for copy in spill_copy(j, rep):
            copy.start()

    own_f[1] = seg_ref[:OWN_GROUPS, :]

    def own_group(g, carry):
        top, best = gather_group(g)
        rank, face = decode(top, best)
        at = pl.ds(g, 1)
        own_f[0, at, :] = top
        own_i[0, at, :] = rank
        own_i[1, at, :] = face
        return carry

    lax.fori_loop(0, OWN_GROUPS, own_group, 0)

    def own_copy(j, source):
        return (
            pltpu.make_async_remote_copy(
                src_ref=own_f, dst_ref=ow_f.at[source],
                send_sem=s_owf.at[j], recv_sem=r_owf.at[source],
                device_id=dev(dom, rep + j), device_id_type=MESH,
            ),
            pltpu.make_async_remote_copy(
                src_ref=own_i, dst_ref=ow_i.at[source],
                send_sem=s_owi.at[j], recv_sem=r_owi.at[source],
                device_id=dev(dom, rep + j), device_id_type=MESH,
            ),
        )

    for j in range(1, n_rep):
        for copy in own_copy(j, rep):
            copy.start()
    ow_f[rep] = own_f[...]
    ow_i[rep] = own_i[...]

    def wait_tot(j, carry):
        tot_dom_in(j).wait_recv()
        return carry

    lax.fori_loop(1, n_dom, wait_tot, 0)

    def add_tot(j, total):
        return total + tot_d[j]

    dom_total = lax.fori_loop(0, n_dom, add_tot, jnp.zeros((SUB, LANES), jnp.float32))
    own_t[...] = dom_total
    tot_r[rep] = dom_total

    def rep_tot(j, source):
        return pltpu.make_async_remote_copy(
            src_ref=own_t, dst_ref=tot_r.at[source],
            send_sem=s_tr.at[j], recv_sem=r_tr.at[source],
            device_id=dev(dom, rep + j), device_id_type=MESH,
        )

    for j in range(1, n_rep):
        rep_tot(j, rep).start()

    def encode(rank, face):
        return jnp.where(rank < 0, KEY_LOW, ((rank - 2) << 30) + (FACE_MASK - face))

    for j in range(1, n_rep):
        rep_tot(j, lax.rem(rep - j + n_rep, n_rep)).wait_recv()
    whole = tot_r[0]
    for r in range(1, n_rep):
        whole = whole + tot_r[r]
    out_mean[0] = jnp.sum(whole[0:1, 0:1]) / jnp.sum(whole[1:2, 0:1])

    for j in range(n_rep):
        for copy in spill_copy(j, lax.rem(rep - j + n_rep, n_rep)):
            copy.wait_recv()
    pen_s, gap_s = sp_f[0, 0], sp_f[0, 1]
    key_s = encode(sp_i[0, 0], sp_i[0, 1])
    for r in range(1, n_rep):
        pen_s = jnp.maximum(pen_s, sp_f[r, 0])
        gap_s = gap_s + sp_f[r, 1]
        key_s = jnp.maximum(key_s, encode(sp_i[r, 0], sp_i[r, 1]))
    for j in range(1, n_rep):
        for copy in own_copy(j, lax.rem(rep - j + n_rep, n_rep)):
            copy.wait_recv()
    pen_o, key_o, gap_o = pen_s, key_s, ow_f[0, 1]
    for r in range(n_rep):
        pen_o = jnp.maximum(pen_o, ow_f[r, 0])
        key_o = jnp.maximum(key_o, encode(ow_i[r, 0], ow_i[r, 1]))
        if r:
            gap_o = gap_o + ow_f[r, 1]
    out_pen[...] = pen_o
    out_key[...] = key_o
    out_gap[...] = gap_o + gap_s

    def end_tot(j, carry):
        tot_dom(j).wait_send()
        return carry

    lax.fori_loop(1, n_dom, end_tot, 0)
    for j in range(1, n_rep):
        rep_tot(j, rep).wait_send()
        for copy in own_copy(j, rep):
            copy.wait_send()
    for j in range(n_rep):
        for copy in spill_copy(j, rep):
            copy.wait_send()


def lane_scratch():
    lane_packs = [
        pltpu.VMEM((DEPTH + SUB, LANES), jnp.int32),
        pltpu.VMEM((DEPTH + SUB, LANES), jnp.float32),
        pltpu.VMEM((DEPTH + SUB, LANES), jnp.int32),
    ]
    lane_accs = [
        pltpu.VMEM((LANES, LANES), jnp.float32),
        pltpu.VMEM((LANES, LANES), jnp.int32),
    ]
    return lane_packs, lane_accs


def dense_call(live, ns, nm, qrow, sec, mst, off, jac, slot, face, rank, block=BLOCK):
    k_size, p_size = ns.shape
    rows = sec.shape[1]
    lines = rows // LANES
    b_lines = block // LANES
    grid = rows // block
    smem = pl.BlockSpec(memory_space=pltpu.SMEM)
    full = lambda shape: pl.BlockSpec(shape, lambda i: (0, 0))
    line_spec = pl.BlockSpec((b_lines, LANES), lambda i: (i, 0))
    wide = pl.BlockSpec((k_size, block), lambda i: (0, i))
    whole = full((lines, LANES))
    padded = full((PAD_GROUPS, LANES))
    lane_packs, lane_accs = lane_scratch()
    return pl.pallas_call(
        dense_kernel,
        grid=(grid,),
        out_shape=(
            jax.ShapeDtypeStruct((k_size, rows), jnp.bfloat16),
            jax.ShapeDtypeStruct((lines, LANES), jnp.float32),
            jax.ShapeDtypeStruct((PAD_GROUPS, LANES), jnp.float32),
            jax.ShapeDtypeStruct((lines, LANES), jnp.int32),
            jax.ShapeDtypeStruct((lines, LANES), jnp.int32),
            jax.ShapeDtypeStruct((PAD_GROUPS, LANES), jnp.float32),
            jax.ShapeDtypeStruct((PAD_GROUPS, LANES), jnp.int32),
        ),
        in_specs=[
            smem, full((k_size, p_size)), full((k_size, p_size)), full((1, p_size)),
            wide, wide, line_spec, line_spec, whole, whole, whole,
        ],
        out_specs=(wide, whole, padded, whole, whole, padded, padded),
        scratch_shapes=[
            pltpu.VMEM((p_size + 16, 2 * k_size), jnp.bfloat16),
            pltpu.VMEM((p_size, LANES), jnp.float32),
            pltpu.VMEM((SUB, LANES), jnp.float32),
            lane_packs,
            *lane_accs,
        ],
        compiler_params=pltpu.CompilerParams(dimension_semantics=("arbitrary",)),
    )(live, ns, nm, qrow, sec, mst, off, jac, slot, face, rank)


def solution(mesh):
    n_dom, n_rep = mesh.shape["dom"], mesh.shape["rep"]

    def shards(ns, nm, sec, mst, off, qw, jac, slot, face, rank, live):
        k_size, p_size = ns.shape
        rows = sec.shape[1]
        lines = rows // LANES

        def lined(x):
            return x.reshape(lines, LANES)

        qrow = qw.reshape(1, p_size)
        off, jac, slot, face, rank = (lined(x) for x in (off, jac, slot, face, rank))
        smem = pl.BlockSpec(memory_space=pltpu.SMEM)
        lane_packs, lane_accs = lane_scratch()
        force, pen, seg, code, key, over_pen, over_key = dense_call(
            live, ns, nm, qrow, sec, mst, off, jac, slot, face, rank
        )

        vmem = pl.BlockSpec(memory_space=pltpu.VMEM)
        tile_f = (2, SUB, LANES)
        sems = pltpu.SemaphoreType.DMA
        best_pen, best_key, gap_sum, mean = pl.pallas_call(
            functools.partial(merge_kernel, n_dom, n_rep),
            out_shape=(
                jax.ShapeDtypeStruct((SUB, LANES), jnp.float32),
                jax.ShapeDtypeStruct((SUB, LANES), jnp.int32),
                jax.ShapeDtypeStruct((SUB, LANES), jnp.float32),
                jax.ShapeDtypeStruct((1,), jnp.float32),
            ),
            in_specs=[smem] + [vmem] * 9,
            out_specs=(vmem, vmem, vmem, smem),
            scratch_shapes=[
                *lane_packs,
                *lane_accs,
                pltpu.VMEM((n_rep,) + tile_f, jnp.float32),
                pltpu.VMEM((n_rep,) + tile_f, jnp.int32),
                pltpu.VMEM((n_rep,) + tile_f, jnp.float32),
                pltpu.VMEM((n_rep,) + tile_f, jnp.int32),
                pltpu.VMEM((n_dom, SUB, LANES), jnp.float32),
                pltpu.VMEM((n_rep, SUB, LANES), jnp.float32),
                pltpu.VMEM((SUB, LANES), jnp.float32),
                pltpu.VMEM(tile_f, jnp.float32),
                pltpu.VMEM(tile_f, jnp.int32),
                pltpu.VMEM((SUB, LANES), jnp.float32),
                pltpu.VMEM(tile_f, jnp.float32),
                pltpu.VMEM(tile_f, jnp.int32),
                pltpu.VMEM((SUB, LANES), jnp.float32),
                sems((n_rep,)), sems((n_rep,)), sems((n_rep,)), sems((n_rep,)),
                sems((n_rep,)), sems((n_rep,)), sems((n_rep,)), sems((n_rep,)),
                sems((n_dom,)), sems((n_dom,)), sems((n_rep,)), sems((n_rep,)),
            ],
            compiler_params=pltpu.CompilerParams(collective_id=0, has_side_effects=True),
        )(live, qrow, slot, code, key, pen, jac, seg, over_pen, over_key)
        best_pen, best_key, gap_sum = (x.reshape(SEG_DEV) for x in (best_pen, best_key, gap_sum))
        none = best_pen < LOWEST_FILL * 0.5
        seg_pen = jnp.where(none, 0.0, best_pen)
        seg_face = jnp.where(none, -1, FACE_MASK - (best_key & FACE_MASK))
        seg_gap = jnp.where(none, 0.0, gap_sum)
        return force, seg_pen, seg_face, seg_gap, mean.reshape(())

    return jax.shard_map(
        shards,
        mesh=mesh,
        in_specs=(
            P(),
            P(),
            P(None, ("dom", "rep")),
            P(None, ("dom", "rep")),
            P(("dom", "rep")),
            P(),
            P(("dom", "rep")),
            P(("dom", "rep")),
            P(("dom", "rep")),
            P(("dom", "rep")),
            P(("dom", "rep")),
        ),
        out_specs=(P(None, ("dom", "rep")), P("dom"), P("dom"), P("dom"), P()),
        check_vma=False,
    )
```

```python
import functools

import jax
import jax.numpy as jnp
from jax import lax
from jax.experimental import pallas as pl
from jax.experimental.pallas import tpu as pltpu
from jax.sharding import PartitionSpec as P

SEG_DEV = 1024
SPILL = 256
LANES = 128
SUB = 8
GROUPS = (SEG_DEV + SPILL) // LANES
OWN_GROUPS = SEG_DEV // LANES
PAD_GROUPS = 16

PENALTY = 400.0
LOWEST_FILL = -1e30
FACE_LIMIT = 1073741824
FACE_MASK = FACE_LIMIT - 1
KEY_LOW = -2147483648
MESH = pl.DeviceIdType.MESH
TILE = 256
DEPTH = 16
BLOCK = 2048


def split3(x):
    a = x.astype(jnp.bfloat16)
    rest = x - a.astype(jnp.float32)
    b = rest.astype(jnp.bfloat16)
    c = (rest - b.astype(jnp.float32)).astype(jnp.bfloat16)
    return a, b, c


def scan_group(g, depth0, depth, code_ref, slot_ref, pen_ref, key_ref, packs, accs_pen, accs_key):
    all_lines = code_ref.shape[0]
    lane_lo, lane_pen, lane_key = packs
    blocks = depth // SUB
    sub = lax.broadcasted_iota(jnp.int32, (SUB, LANES), 0)
    wants = [(sub + (depth0 + SUB * b)) * PAD_GROUPS + g for b in range(blocks)]

    def pull(i, carry):
        los, pens, keys = (list(part) for part in carry)
        code = code_ref[pl.ds(i, SUB, stride=0), :]
        slot = slot_ref[pl.ds(i, SUB, stride=0), :]
        pen = pen_ref[pl.ds(i, SUB, stride=0), :]
        key = key_ref[pl.ds(i, SUB, stride=0), :]
        for b in range(blocks):
            hit = code == wants[b]
            los[b] = jnp.where(hit, slot, los[b])
            pens[b] = jnp.where(hit, pen, pens[b])
            keys[b] = jnp.where(hit, key, keys[b])
        return tuple(los), tuple(pens), tuple(keys)

    none = jnp.full((SUB, LANES), -1, jnp.int32)
    empty = jnp.full((SUB, LANES), LOWEST_FILL, jnp.float32)
    start = ((none,) * blocks, (empty,) * blocks, (none,) * blocks)
    los, pens, keys = lax.fori_loop(0, all_lines, pull, start, unroll=8)
    for b in range(blocks):
        rows = slice(SUB * b, SUB * (b + 1))
        lane_lo[rows, :] = los[b]
        lane_pen[rows, :] = pens[b]
        lane_key[rows, :] = keys[b]

    tiles = LANES // SUB
    half = tiles // 2
    for part in range(2):
        marks = [sub + (g * LANES + SUB * (part * half + q)) for q in range(half)]
        best_pen = [empty] * half
        best_key = [jnp.full((SUB, LANES), KEY_LOW, jnp.int32)] * half
        for j in range(depth):
            lo = lane_lo[pl.ds(j, SUB, stride=0), :]
            pen = lane_pen[pl.ds(j, SUB, stride=0), :]
            key = lane_key[pl.ds(j, SUB, stride=0), :]
            for q in range(half):
                hit = lo == marks[q]
                best_pen[q] = jnp.maximum(best_pen[q], jnp.where(hit, pen, LOWEST_FILL))
                best_key[q] = jnp.maximum(best_key[q], jnp.where(hit, key, KEY_LOW))
        for q in range(half):
            rows = slice(SUB * (part * half + q), SUB * (part * half + q + 1))
            accs_pen[rows, :] = best_pen[q]
            accs_key[rows, :] = best_key[q]
    top = jnp.max(accs_pen[...].T, axis=0, keepdims=True)
    best = jnp.max(accs_key[...].T, axis=0, keepdims=True)
    return top, best


def dense_kernel(
    live_ref, ns_ref, nm_ref, qw_ref, sec_ref, mst_ref, off_ref, jac_ref, slot_ref,
    face_ref, rank_ref,
    force_ref, pen_ref, seg_ref, code_ref, key_ref, over_pen, over_key,
    wt_ref, nq_ref, packs, accs_pen, accs_key,
):
    step = pl.program_id(0)
    all_lines = slot_ref.shape[0]
    k_size, p_size = ns_ref.shape
    rows = sec_ref.shape[1]
    lines = rows // LANES
    per_tile = TILE // LANES

    @pl.when(step == 0)
    def _():
        w = jnp.concatenate([ns_ref[...], -nm_ref[...]], axis=0).astype(jnp.float32)
        qrow = qw_ref[...]
        wt = w.T
        qmat = jnp.broadcast_to(qrow, (LANES, p_size)).T
        v = jnp.sum(wt * qmat, axis=0, keepdims=True)
        qsum = jnp.sum(qmat, axis=0, keepdims=True)
        depth = wt_ref.shape[1]
        pick = lax.broadcasted_iota(jnp.int32, (16, depth), 0)
        column = lax.broadcasted_iota(jnp.int32, (p_size, depth - 2 * k_size), 1)
        wt_ref[0:p_size, 0 : 2 * k_size] = wt.astype(jnp.bfloat16)
        wt_ref[0:p_size, 2 * k_size :] = jnp.where(column < 3, 1.0, 0.0).astype(jnp.bfloat16)
        lane_row = lax.broadcasted_iota(jnp.int32, (1, LANES), 1)
        tail = jnp.where(lane_row < 3, qsum, 0.0)[:, : depth - 2 * k_size]
        a, b, c = (part.astype(jnp.float32) for part in split3(jnp.concatenate([v, tail], axis=1)))
        stacked = jnp.where(
            pick == 0, a, jnp.where(pick == 1, b, jnp.where(pick == 2, c, 0.0))
        )
        wt_ref[p_size:, :] = stacked.astype(jnp.bfloat16)
        scaled = ns_ref[...].astype(jnp.float32) * qrow
        top = scaled.astype(jnp.bfloat16)
        low = (scaled - top.astype(jnp.float32)).astype(jnp.bfloat16)
        nq_ref[...] = jnp.concatenate([top, low], axis=0)
        seg_ref[...] = jnp.zeros_like(seg_ref)
        over_pen[...] = jnp.full(over_pen.shape, LOWEST_FILL, jnp.float32)
        over_key[...] = jnp.full(over_key.shape, KEY_LOW, jnp.int32)
        row_id = (
            lax.broadcasted_iota(jnp.int32, (all_lines, LANES), 0) * LANES
            + lax.broadcasted_iota(jnp.int32, (all_lines, LANES), 1)
        )
        alive = row_id < live_ref[0]
        key_ref[...] = ((rank_ref[...] - 2) << 30) + (FACE_MASK - face_ref[...])
        group = jnp.where(alive, slot_ref[...] >> 7, -1)
        before = (
            lax.broadcasted_iota(jnp.int32, (all_lines, all_lines), 1)
            < lax.broadcasted_iota(jnp.int32, (all_lines, all_lines), 0)
        )
        before = jnp.where(before, 1.0, 0.0).astype(jnp.bfloat16)
        code = jnp.full((all_lines, LANES), -1, jnp.int32)
        for g in range(GROUPS):
            mine = group == g
            place = jnp.dot(
                before, jnp.where(mine, 1.0, 0.0).astype(jnp.bfloat16),
                preferred_element_type=jnp.float32,
            ).astype(jnp.int32)
            code = jnp.where(mine, place * PAD_GROUPS + g, code)
        code_ref[...] = code

    live_count = live_ref[0]
    first = step * rows
    line0 = step * lines
    wt = wt_ref[...]
    nq = nq_ref[...]
    seg_total = jnp.zeros((PAD_GROUPS, LANES), jnp.float32)
    pad_rows = wt.shape[1] - 2 * k_size
    pad_id = lax.broadcasted_iota(jnp.int32, (pad_rows, TILE), 0)

    def line_of(ref, at, count):
        return jnp.concatenate([ref[pl.ds(at + i, 1), :] for i in range(count)], axis=1)

    def project(tile):
        cols = pl.ds(tile * TILE, TILE)
        offset = line_of(off_ref, tile * per_tile, per_tile)
        a, b, c = (part.astype(jnp.float32) for part in split3(offset))
        extra = jnp.where(pad_id == 0, a, jnp.where(pad_id == 1, b, jnp.where(pad_id == 2, c, 0.0)))
        x = jnp.concatenate([sec_ref[:, cols], mst_ref[:, cols], extra.astype(jnp.bfloat16)], axis=0)
        return jnp.dot(wt, x, preferred_element_type=jnp.float32)

    row_lane = lax.broadcasted_iota(jnp.int32, (1, TILE), 1)
    hi_id = lax.broadcasted_iota(jnp.int32, (PAD_GROUPS, TILE), 0)
    lo_id = lax.broadcasted_iota(jnp.int32, (LANES, TILE), 0)
    tiles = rows // TILE
    field = project(0)
    for tile in range(tiles):
        cols = pl.ds(tile * TILE, TILE)
        coming = project(tile + 1) if tile + 1 < tiles else None
        gap = field[:p_size]
        live = (row_lane + (first + tile * TILE)) < live_count
        jac_live = jnp.where(live, line_of(jac_ref, tile * per_tile, per_tile), 0.0)
        load = jnp.minimum(gap.astype(jnp.bfloat16), 0)
        force = jnp.dot(nq, load, preferred_element_type=jnp.float32)
        force_ref[:, cols] = (
            (force[:k_size] + force[k_size:]) * (jac_live * -PENALTY)
        ).astype(jnp.bfloat16)
        pen = jnp.where(live, -jnp.min(gap, axis=0, keepdims=True), LOWEST_FILL)
        for part in range(per_tile):
            pen_ref[pl.ds(line0 + tile * per_tile + part, 1), :] = pen[:, part * LANES : (part + 1) * LANES]
        row_gap = jac_live * jnp.sum(field[p_size : p_size + SUB], axis=0, keepdims=True)
        slot = line_of(slot_ref, line0 + tile * per_tile, per_tile)
        spread = jnp.where(hi_id == (slot >> 7), row_gap, 0.0)
        left = jnp.concatenate(split3(spread), axis=0)
        right = jnp.where(lo_id == (slot & (LANES - 1)), 1.0, 0.0).astype(jnp.bfloat16)
        got = lax.dot_general(
            left, right, (((1,), (1,)), ((), ())), preferred_element_type=jnp.float32
        )
        seg_total = seg_total + (
            got[0:PAD_GROUPS] + got[PAD_GROUPS : 2 * PAD_GROUPS] + got[2 * PAD_GROUPS :]
        )
        field = coming
    seg_ref[...] += seg_total

    @pl.when(step == pl.num_programs(0) - 1)
    def _():
        def one(worst):
            code = code_ref[...]
            g = worst & (PAD_GROUPS - 1)
            low = (worst >> 4) & -SUB
            top, best = scan_group(
                g, low, SUB, code_ref, slot_ref, pen_ref, key_ref, packs, accs_pen, accs_key
            )
            at = pl.ds(g, 1)
            over_pen[at, :] = jnp.maximum(over_pen[at, :], top)
            over_key[at, :] = jnp.maximum(over_key[at, :], best)
            done = ((code & (PAD_GROUPS - 1)) == g) & (code >= low * PAD_GROUPS)
            code = jnp.where(done, -1, code)
            code_ref[...] = code
            return jnp.max(code)

        lax.while_loop(lambda worst: worst >= DEPTH * PAD_GROUPS, one, jnp.max(code_ref[...]))


def merge_kernel(
    n_dom, n_rep,
    live_ref, qw_ref, slot_ref, code_ref, key_ref, pen_ref, jac_ref, seg_ref, over_pen, over_key,
    out_pen, out_key, out_gap, out_mean,
    lane_lo, lane_pen, lane_key, accs_pen, accs_key,
    sp_f, sp_i, ow_f, ow_i, tot_d, tot_s,
    spill_f, spill_i, own_f, own_i,
    s_spf, r_spf, s_spi, r_spi, s_owf, r_owf, s_owi, r_owi, s_td, r_td,
):
    dom = lax.axis_index("dom")
    rep = lax.axis_index("rep")
    lines = slot_ref.shape[0]

    def dev(d, r):
        return {"dom": lax.rem(d + n_dom, n_dom), "rep": lax.rem(r + n_rep, n_rep)}

    barrier = pltpu.get_barrier_semaphore()

    def greet(d, r):
        pl.semaphore_signal(barrier, inc=1, device_id=dev(d, r), device_id_type=MESH)

    count = n_dom * n_rep
    me = dom * n_rep + rep

    def peer(j):
        flat = lax.rem(me + j, count)
        return lax.div(flat, n_rep), lax.rem(flat, n_rep)

    def greet_peer(j, carry):
        greet(*peer(j))
        return carry

    lax.fori_loop(1, count, greet_peer, 0)

    live_count = live_ref[0]
    row_id = (
        lax.broadcasted_iota(jnp.int32, (lines, LANES), 0) * LANES
        + lax.broadcasted_iota(jnp.int32, (lines, LANES), 1)
    )
    live = row_id < live_count
    total_gap = jnp.sum(jnp.sum(seg_ref[...], axis=0, keepdims=True), axis=1, keepdims=True)
    area_rows = jnp.where(live, jac_ref[...], 0.0)
    total_area = jnp.sum(
        jnp.sum(area_rows, axis=0, keepdims=True), axis=1, keepdims=True
    ) * jnp.sum(qw_ref[...], axis=1, keepdims=True)
    lane = lax.broadcasted_iota(jnp.int32, (1, LANES), 1)
    pair = jnp.where(lane == 0, total_gap, jnp.where(lane == 1, total_area, 0.0))
    tot_s[...] = pair
    tot_d[me] = pair

    def tot_copy(j, source):
        return pltpu.make_async_remote_copy(
            src_ref=tot_s, dst_ref=tot_d.at[source],
            send_sem=s_td.at[j], recv_sem=r_td.at[source],
            device_id=dev(*peer(j)), device_id_type=MESH,
        )

    def start_tot(j, carry):
        tot_copy(j, me).start()
        return carry

    def gather_group(g):
        top, best = scan_group(
            g, 0, DEPTH, code_ref, slot_ref, pen_ref, key_ref,
            (lane_lo, lane_pen, lane_key), accs_pen, accs_key,
        )
        at = pl.ds(g, 1)
        return jnp.maximum(top, over_pen[at, :]), jnp.maximum(best, over_key[at, :])

    def decode(top, best):
        none = top < LOWEST_FILL * 0.5
        rank = jnp.where(none, -1, (best >> 30) + 2)
        face = jnp.where(none, FACE_LIMIT, FACE_MASK - (best & FACE_MASK))
        return rank, face

    spill_f[0] = jnp.full((SUB, LANES), LOWEST_FILL, jnp.float32)
    spill_i[0] = jnp.full((SUB, LANES), -1, jnp.int32)
    spill_i[1] = jnp.full((SUB, LANES), FACE_LIMIT, jnp.int32)
    spill_f[1] = seg_ref[OWN_GROUPS:, :]
    def spill_group(g, carry):
        top, best = gather_group(g)
        rank, face = decode(top, best)
        at = pl.ds(g - OWN_GROUPS, 1)
        spill_f[0, at, :] = top
        spill_i[0, at, :] = rank
        spill_i[1, at, :] = face
        return carry

    lax.fori_loop(OWN_GROUPS, GROUPS, spill_group, 0)

    pl.semaphore_wait(barrier, count - 1)

    lax.fori_loop(1, count, start_tot, 0)

    def spill_copy(j, source):
        return (
            pltpu.make_async_remote_copy(
                src_ref=spill_f, dst_ref=sp_f.at[source],
                send_sem=s_spf.at[j], recv_sem=r_spf.at[source],
                device_id=dev(dom + 1, rep + j), device_id_type=MESH,
            ),
            pltpu.make_async_remote_copy(
                src_ref=spill_i, dst_ref=sp_i.at[source],
                send_sem=s_spi.at[j], recv_sem=r_spi.at[source],
                device_id=dev(dom + 1, rep + j), device_id_type=MESH,
            ),
        )

    for j in range(n_rep):
        for copy in spill_copy(j, rep):
            copy.start()

    own_f[1] = seg_ref[:OWN_GROUPS, :]

    def own_group(g, carry):
        top, best = gather_group(g)
        rank, face = decode(top, best)
        at = pl.ds(g, 1)
        own_f[0, at, :] = top
        own_i[0, at, :] = rank
        own_i[1, at, :] = face
        return carry

    lax.fori_loop(0, OWN_GROUPS, own_group, 0)

    def own_copy(j, source):
        return (
            pltpu.make_async_remote_copy(
                src_ref=own_f, dst_ref=ow_f.at[source],
                send_sem=s_owf.at[j], recv_sem=r_owf.at[source],
                device_id=dev(dom, rep + j), device_id_type=MESH,
            ),
            pltpu.make_async_remote_copy(
                src_ref=own_i, dst_ref=ow_i.at[source],
                send_sem=s_owi.at[j], recv_sem=r_owi.at[source],
                device_id=dev(dom, rep + j), device_id_type=MESH,
            ),
        )

    for j in range(1, n_rep):
        for copy in own_copy(j, rep):
            copy.start()
    ow_f[rep] = own_f[...]
    ow_i[rep] = own_i[...]

    def encode(rank, face):
        return jnp.where(rank < 0, KEY_LOW, ((rank - 2) << 30) + (FACE_MASK - face))

    def wait_tot(j, carry):
        tot_copy(j, lax.rem(me - j + count, count)).wait_recv()
        return carry

    lax.fori_loop(1, count, wait_tot, 0)

    def add_tot(j, total):
        return total + tot_d[j]

    whole = lax.fori_loop(0, count, add_tot, jnp.zeros((1, LANES), jnp.float32))
    out_mean[0] = jnp.sum(whole[:, 0:1]) / jnp.sum(whole[:, 1:2])

    for j in range(n_rep):
        for copy in spill_copy(j, lax.rem(rep - j + n_rep, n_rep)):
            copy.wait_recv()
    pen_s, gap_s = sp_f[0, 0], sp_f[0, 1]
    key_s = encode(sp_i[0, 0], sp_i[0, 1])
    for r in range(1, n_rep):
        pen_s = jnp.maximum(pen_s, sp_f[r, 0])
        gap_s = gap_s + sp_f[r, 1]
        key_s = jnp.maximum(key_s, encode(sp_i[r, 0], sp_i[r, 1]))
    for j in range(1, n_rep):
        for copy in own_copy(j, lax.rem(rep - j + n_rep, n_rep)):
            copy.wait_recv()
    pen_o, key_o, gap_o = pen_s, key_s, ow_f[0, 1]
    for r in range(n_rep):
        pen_o = jnp.maximum(pen_o, ow_f[r, 0])
        key_o = jnp.maximum(key_o, encode(ow_i[r, 0], ow_i[r, 1]))
        if r:
            gap_o = gap_o + ow_f[r, 1]
    out_pen[...] = pen_o
    out_key[...] = key_o
    out_gap[...] = gap_o + gap_s

    def end_tot(j, carry):
        tot_copy(j, me).wait_send()
        return carry

    lax.fori_loop(1, count, end_tot, 0)
    for j in range(1, n_rep):
        for copy in own_copy(j, rep):
            copy.wait_send()
    for j in range(n_rep):
        for copy in spill_copy(j, rep):
            copy.wait_send()


def lane_scratch():
    lane_packs = [
        pltpu.VMEM((DEPTH + SUB, LANES), jnp.int32),
        pltpu.VMEM((DEPTH + SUB, LANES), jnp.float32),
        pltpu.VMEM((DEPTH + SUB, LANES), jnp.int32),
    ]
    lane_accs = [
        pltpu.VMEM((LANES, LANES), jnp.float32),
        pltpu.VMEM((LANES, LANES), jnp.int32),
    ]
    return lane_packs, lane_accs


def dense_call(live, ns, nm, qrow, sec, mst, off, jac, slot, face, rank, block=BLOCK):
    k_size, p_size = ns.shape
    rows = sec.shape[1]
    lines = rows // LANES
    b_lines = block // LANES
    grid = rows // block
    smem = pl.BlockSpec(memory_space=pltpu.SMEM)
    full = lambda shape: pl.BlockSpec(shape, lambda i: (0, 0))
    line_spec = pl.BlockSpec((b_lines, LANES), lambda i: (i, 0))
    wide = pl.BlockSpec((k_size, block), lambda i: (0, i))
    whole = full((lines, LANES))
    padded = full((PAD_GROUPS, LANES))
    lane_packs, lane_accs = lane_scratch()
    return pl.pallas_call(
        dense_kernel,
        grid=(grid,),
        out_shape=(
            jax.ShapeDtypeStruct((k_size, rows), jnp.bfloat16),
            jax.ShapeDtypeStruct((lines, LANES), jnp.float32),
            jax.ShapeDtypeStruct((PAD_GROUPS, LANES), jnp.float32),
            jax.ShapeDtypeStruct((lines, LANES), jnp.int32),
            jax.ShapeDtypeStruct((lines, LANES), jnp.int32),
            jax.ShapeDtypeStruct((PAD_GROUPS, LANES), jnp.float32),
            jax.ShapeDtypeStruct((PAD_GROUPS, LANES), jnp.int32),
        ),
        in_specs=[
            smem, full((k_size, p_size)), full((k_size, p_size)), full((1, p_size)),
            wide, wide, line_spec, line_spec, whole, whole, whole,
        ],
        out_specs=(wide, whole, padded, whole, whole, padded, padded),
        scratch_shapes=[
            pltpu.VMEM((p_size + 16, 2 * k_size + 16), jnp.bfloat16),
            pltpu.VMEM((2 * k_size, p_size), jnp.bfloat16),
            lane_packs,
            *lane_accs,
        ],
        compiler_params=pltpu.CompilerParams(dimension_semantics=("arbitrary",)),
    )(live, ns, nm, qrow, sec, mst, off, jac, slot, face, rank)


def solution(mesh):
    n_dom, n_rep = mesh.shape["dom"], mesh.shape["rep"]

    def shards(ns, nm, sec, mst, off, qw, jac, slot, face, rank, live):
        k_size, p_size = ns.shape
        rows = sec.shape[1]
        lines = rows // LANES

        def lined(x):
            return x.reshape(lines, LANES)

        qrow = qw.reshape(1, p_size)
        off, jac, slot, face, rank = (lined(x) for x in (off, jac, slot, face, rank))
        smem = pl.BlockSpec(memory_space=pltpu.SMEM)
        lane_packs, lane_accs = lane_scratch()
        force, pen, seg, code, key, over_pen, over_key = dense_call(
            live, ns, nm, qrow, sec, mst, off, jac, slot, face, rank
        )

        vmem = pl.BlockSpec(memory_space=pltpu.VMEM)
        tile_f = (2, SUB, LANES)
        sems = pltpu.SemaphoreType.DMA
        best_pen, best_key, gap_sum, mean = pl.pallas_call(
            functools.partial(merge_kernel, n_dom, n_rep),
            out_shape=(
                jax.ShapeDtypeStruct((SUB, LANES), jnp.float32),
                jax.ShapeDtypeStruct((SUB, LANES), jnp.int32),
                jax.ShapeDtypeStruct((SUB, LANES), jnp.float32),
                jax.ShapeDtypeStruct((1,), jnp.float32),
            ),
            in_specs=[smem] + [vmem] * 9,
            out_specs=(vmem, vmem, vmem, smem),
            scratch_shapes=[
                *lane_packs,
                *lane_accs,
                pltpu.VMEM((n_rep,) + tile_f, jnp.float32),
                pltpu.VMEM((n_rep,) + tile_f, jnp.int32),
                pltpu.VMEM((n_rep,) + tile_f, jnp.float32),
                pltpu.VMEM((n_rep,) + tile_f, jnp.int32),
                pltpu.VMEM((n_dom * n_rep, 1, LANES), jnp.float32),
                pltpu.VMEM((1, LANES), jnp.float32),
                pltpu.VMEM(tile_f, jnp.float32),
                pltpu.VMEM(tile_f, jnp.int32),
                pltpu.VMEM(tile_f, jnp.float32),
                pltpu.VMEM(tile_f, jnp.int32),
                sems((n_rep,)), sems((n_rep,)), sems((n_rep,)), sems((n_rep,)),
                sems((n_rep,)), sems((n_rep,)), sems((n_rep,)), sems((n_rep,)),
                sems((n_dom * n_rep,)), sems((n_dom * n_rep,)),
            ],
            compiler_params=pltpu.CompilerParams(collective_id=0, has_side_effects=True),
        )(live, qrow, slot, code, key, pen, jac, seg, over_pen, over_key)
        best_pen, best_key, gap_sum = (x.reshape(SEG_DEV) for x in (best_pen, best_key, gap_sum))
        none = best_pen < LOWEST_FILL * 0.5
        seg_pen = jnp.where(none, 0.0, best_pen)
        seg_face = jnp.where(none, -1, FACE_MASK - (best_key & FACE_MASK))
        seg_gap = jnp.where(none, 0.0, gap_sum)
        return force, seg_pen, seg_face, seg_gap, mean.reshape(())

    return jax.shard_map(
        shards,
        mesh=mesh,
        in_specs=(
            P(),
            P(),
            P(None, ("dom", "rep")),
            P(None, ("dom", "rep")),
            P(("dom", "rep")),
            P(),
            P(("dom", "rep")),
            P(("dom", "rep")),
            P(("dom", "rep")),
            P(("dom", "rep")),
            P(("dom", "rep")),
        ),
        out_specs=(P(None, ("dom", "rep")), P("dom"), P("dom"), P("dom"), P()),
        check_vma=False,
    )
```

```python
import functools

import jax
import jax.numpy as jnp
from jax import lax
from jax.experimental import pallas as pl
from jax.experimental.pallas import tpu as pltpu
from jax.sharding import PartitionSpec as P

SEG_DEV = 1024
SPILL = 256
LANES = 128
SUB = 8
GROUPS = (SEG_DEV + SPILL) // LANES
OWN_GROUPS = SEG_DEV // LANES
PAD_GROUPS = 16

PENALTY = 400.0
LOWEST_FILL = -1e30
FACE_LIMIT = 1073741824
FACE_MASK = FACE_LIMIT - 1
KEY_LOW = -2147483648
MESH = pl.DeviceIdType.MESH
TILE = 256
DEPTH = 16
BLOCK = 2048


def split3(x):
    a = x.astype(jnp.bfloat16)
    rest = x - a.astype(jnp.float32)
    b = rest.astype(jnp.bfloat16)
    c = (rest - b.astype(jnp.float32)).astype(jnp.bfloat16)
    return a, b, c


def scan_group(g, depth0, depth, code_ref, slot_ref, pen_ref, key_ref, packs, accs_pen, accs_key):
    all_lines = code_ref.shape[0]
    lane_lo, lane_pen, lane_key = packs
    blocks = depth // SUB
    sub = lax.broadcasted_iota(jnp.int32, (SUB, LANES), 0)
    wants = [(sub + (depth0 + SUB * b)) * PAD_GROUPS + g for b in range(blocks)]

    def pull(i, carry):
        los, pens, keys = (list(part) for part in carry)
        code = code_ref[pl.ds(i, SUB, stride=0), :]
        slot = slot_ref[pl.ds(i, SUB, stride=0), :]
        pen = pen_ref[pl.ds(i, SUB, stride=0), :]
        key = key_ref[pl.ds(i, SUB, stride=0), :]
        for b in range(blocks):
            hit = code == wants[b]
            los[b] = jnp.where(hit, slot, los[b])
            pens[b] = jnp.where(hit, pen, pens[b])
            keys[b] = jnp.where(hit, key, keys[b])
        return tuple(los), tuple(pens), tuple(keys)

    none = jnp.full((SUB, LANES), -1, jnp.int32)
    empty = jnp.full((SUB, LANES), LOWEST_FILL, jnp.float32)
    start = ((none,) * blocks, (empty,) * blocks, (none,) * blocks)
    los, pens, keys = lax.fori_loop(0, all_lines, pull, start, unroll=8)
    for b in range(blocks):
        rows = slice(SUB * b, SUB * (b + 1))
        lane_lo[rows, :] = los[b]
        lane_pen[rows, :] = pens[b]
        lane_key[rows, :] = keys[b]

    tiles = LANES // SUB
    half = tiles // 2
    for part in range(2):
        marks = [sub + (g * LANES + SUB * (part * half + q)) for q in range(half)]
        best_pen = [empty] * half
        best_key = [jnp.full((SUB, LANES), KEY_LOW, jnp.int32)] * half
        for j in range(depth):
            lo = lane_lo[pl.ds(j, SUB, stride=0), :]
            pen = lane_pen[pl.ds(j, SUB, stride=0), :]
            key = lane_key[pl.ds(j, SUB, stride=0), :]
            for q in range(half):
                hit = lo == marks[q]
                best_pen[q] = jnp.maximum(best_pen[q], jnp.where(hit, pen, LOWEST_FILL))
                best_key[q] = jnp.maximum(best_key[q], jnp.where(hit, key, KEY_LOW))
        for q in range(half):
            rows = slice(SUB * (part * half + q), SUB * (part * half + q + 1))
            accs_pen[rows, :] = best_pen[q]
            accs_key[rows, :] = best_key[q]
    top = jnp.max(accs_pen[...].T, axis=0, keepdims=True)
    best = jnp.max(accs_key[...].T, axis=0, keepdims=True)
    return top, best


def dense_kernel(
    live_ref, ns_ref, nm_ref, qw_ref, sec_ref, mst_ref, off_ref, jac_ref, slot_ref,
    face_ref, rank_ref,
    force_ref, pen_ref, seg_ref, code_ref, key_ref, over_pen, over_key,
    wt_ref, nq_ref, packs, accs_pen, accs_key,
):
    step = pl.program_id(0)
    all_lines = slot_ref.shape[0]
    k_size, p_size = ns_ref.shape
    rows = sec_ref.shape[1]
    lines = rows // LANES
    per_tile = TILE // LANES

    @pl.when(step == 0)
    def _():
        w = jnp.concatenate([ns_ref[...], -nm_ref[...]], axis=0).astype(jnp.float32)
        qrow = qw_ref[...]
        wt = w.T
        qmat = jnp.broadcast_to(qrow, (LANES, p_size)).T
        v = jnp.sum(wt * qmat, axis=0, keepdims=True)
        qsum = jnp.sum(qmat, axis=0, keepdims=True)
        depth = wt_ref.shape[1]
        pick = lax.broadcasted_iota(jnp.int32, (16, depth), 0)
        column = lax.broadcasted_iota(jnp.int32, (p_size, depth - 2 * k_size), 1)
        wt_ref[0:p_size, 0 : 2 * k_size] = wt.astype(jnp.bfloat16)
        wt_ref[0:p_size, 2 * k_size :] = jnp.where(column < 3, 1.0, 0.0).astype(jnp.bfloat16)
        lane_row = lax.broadcasted_iota(jnp.int32, (1, LANES), 1)
        tail = jnp.where(lane_row < 3, qsum, 0.0)[:, : depth - 2 * k_size]
        a, b, c = (part.astype(jnp.float32) for part in split3(jnp.concatenate([v, tail], axis=1)))
        stacked = jnp.where(
            pick == 0, a, jnp.where(pick == 1, b, jnp.where(pick == 2, c, 0.0))
        )
        wt_ref[p_size:, :] = stacked.astype(jnp.bfloat16)
        scaled = ns_ref[...].astype(jnp.float32) * qrow
        top = scaled.astype(jnp.bfloat16)
        low = (scaled - top.astype(jnp.float32)).astype(jnp.bfloat16)
        nq_ref[...] = jnp.concatenate([top, low], axis=0)
        seg_ref[...] = jnp.zeros_like(seg_ref)
        over_pen[...] = jnp.full(over_pen.shape, LOWEST_FILL, jnp.float32)
        over_key[...] = jnp.full(over_key.shape, KEY_LOW, jnp.int32)
        row_id = (
            lax.broadcasted_iota(jnp.int32, (all_lines, LANES), 0) * LANES
            + lax.broadcasted_iota(jnp.int32, (all_lines, LANES), 1)
        )
        alive = row_id < live_ref[0]
        key_ref[...] = ((rank_ref[...] - 2) << 30) + (FACE_MASK - face_ref[...])
        group = jnp.where(alive, slot_ref[...] >> 7, -1)
        before = (
            lax.broadcasted_iota(jnp.int32, (all_lines, all_lines), 1)
            < lax.broadcasted_iota(jnp.int32, (all_lines, all_lines), 0)
        )
        before = jnp.where(before, 1.0, 0.0).astype(jnp.bfloat16)
        code = jnp.full((all_lines, LANES), -1, jnp.int32)
        for g in range(GROUPS):
            mine = group == g
            place = jnp.dot(
                before, jnp.where(mine, 1.0, 0.0).astype(jnp.bfloat16),
                preferred_element_type=jnp.float32,
            ).astype(jnp.int32)
            code = jnp.where(mine, place * PAD_GROUPS + g, code)
        code_ref[...] = code

    live_count = live_ref[0]
    first = step * rows
    line0 = step * lines
    wt = wt_ref[...]
    nq = nq_ref[...]
    seg_total = jnp.zeros((PAD_GROUPS, LANES), jnp.float32)
    pad_rows = wt.shape[1] - 2 * k_size
    pad_id = lax.broadcasted_iota(jnp.int32, (pad_rows, TILE), 0)

    def line_of(ref, at, count):
        return jnp.concatenate([ref[pl.ds(at + i, 1), :] for i in range(count)], axis=1)

    def project(tile):
        cols = pl.ds(tile * TILE, TILE)
        offset = line_of(off_ref, tile * per_tile, per_tile)
        a, b, c = (part.astype(jnp.float32) for part in split3(offset))
        extra = jnp.where(pad_id == 0, a, jnp.where(pad_id == 1, b, jnp.where(pad_id == 2, c, 0.0)))
        x = jnp.concatenate([sec_ref[:, cols], mst_ref[:, cols], extra.astype(jnp.bfloat16)], axis=0)
        return jnp.dot(wt, x, preferred_element_type=jnp.float32)

    row_lane = lax.broadcasted_iota(jnp.int32, (1, TILE), 1)
    hi_id = lax.broadcasted_iota(jnp.int32, (PAD_GROUPS, TILE), 0)
    lo_id = lax.broadcasted_iota(jnp.int32, (LANES, TILE), 0)
    tiles = rows // TILE
    field = project(0)
    for tile in range(tiles):
        cols = pl.ds(tile * TILE, TILE)
        coming = project(tile + 1) if tile + 1 < tiles else None
        gap = field[:p_size]
        live = (row_lane + (first + tile * TILE)) < live_count
        jac_live = jnp.where(live, line_of(jac_ref, tile * per_tile, per_tile), 0.0)
        load = jnp.minimum(gap.astype(jnp.bfloat16), 0)
        force = jnp.dot(nq, load, preferred_element_type=jnp.float32)
        force_ref[:, cols] = (
            (force[:k_size] + force[k_size:]) * (jac_live * -PENALTY)
        ).astype(jnp.bfloat16)
        pen = jnp.where(live, -jnp.min(gap, axis=0, keepdims=True), LOWEST_FILL)
        for part in range(per_tile):
            pen_ref[pl.ds(line0 + tile * per_tile + part, 1), :] = pen[:, part * LANES : (part + 1) * LANES]
        row_gap = jac_live * jnp.sum(field[p_size : p_size + SUB], axis=0, keepdims=True)
        slot = line_of(slot_ref, line0 + tile * per_tile, per_tile)
        spread = jnp.where(hi_id == (slot >> 7), row_gap, 0.0)
        left = jnp.concatenate(split3(spread), axis=0)
        right = jnp.where(lo_id == (slot & (LANES - 1)), 1.0, 0.0).astype(jnp.bfloat16)
        got = lax.dot_general(
            left, right, (((1,), (1,)), ((), ())), preferred_element_type=jnp.float32
        )
        seg_total = seg_total + (
            got[0:PAD_GROUPS] + got[PAD_GROUPS : 2 * PAD_GROUPS] + got[2 * PAD_GROUPS :]
        )
        field = coming
    seg_ref[...] += seg_total

    @pl.when(step == pl.num_programs(0) - 1)
    def _():
        def one(worst):
            code = code_ref[...]
            g = worst & (PAD_GROUPS - 1)
            low = (worst >> 4) & -SUB
            top, best = scan_group(
                g, low, SUB, code_ref, slot_ref, pen_ref, key_ref, packs, accs_pen, accs_key
            )
            at = pl.ds(g, 1)
            over_pen[at, :] = jnp.maximum(over_pen[at, :], top)
            over_key[at, :] = jnp.maximum(over_key[at, :], best)
            done = ((code & (PAD_GROUPS - 1)) == g) & (code >= low * PAD_GROUPS)
            code = jnp.where(done, -1, code)
            code_ref[...] = code
            return jnp.max(code)

        lax.while_loop(lambda worst: worst >= DEPTH * PAD_GROUPS, one, jnp.max(code_ref[...]))


def merge_kernel(
    n_dom, n_rep,
    live_ref, qw_ref, slot_h, code_h, key_h, pen_h, jac_h, seg_h, over_pen_h, over_key_h,
    out_pen, out_key, out_gap, out_mean,
    slot_ref, code_ref, key_ref, pen_ref, jac_ref, seg_ref, over_pen, over_key, s_in,
    lane_lo, lane_pen, lane_key, accs_pen, accs_key,
    sp_f, sp_i, ow_f, ow_i, tot_d, tot_s,
    spill_f, spill_i, own_f, own_i,
    s_spf, r_spf, s_spi, r_spi, s_owf, r_owf, s_owi, r_owi, s_td, r_td,
):
    dom = lax.axis_index("dom")
    rep = lax.axis_index("rep")
    lines = slot_ref.shape[0]

    def dev(d, r):
        return {"dom": lax.rem(d + n_dom, n_dom), "rep": lax.rem(r + n_rep, n_rep)}

    barrier = pltpu.get_barrier_semaphore()

    def greet(d, r):
        pl.semaphore_signal(barrier, inc=1, device_id=dev(d, r), device_id_type=MESH)

    count = n_dom * n_rep
    me = dom * n_rep + rep

    def peer(j):
        flat = lax.rem(me + j, count)
        return lax.div(flat, n_rep), lax.rem(flat, n_rep)

    def greet_peer(j, carry):
        greet(*peer(j))
        return carry

    lax.fori_loop(1, count, greet_peer, 0)
    loads = [
        pltpu.make_async_copy(source, held, s_in.at[i])
        for i, (source, held) in enumerate((
            (slot_h, slot_ref), (code_h, code_ref), (key_h, key_ref), (pen_h, pen_ref),
            (jac_h, jac_ref), (seg_h, seg_ref), (over_pen_h, over_pen), (over_key_h, over_key),
        ))
    ]
    for copy in loads:
        copy.start()
    for copy in loads:
        copy.wait()

    live_count = live_ref[0]
    row_id = (
        lax.broadcasted_iota(jnp.int32, (lines, LANES), 0) * LANES
        + lax.broadcasted_iota(jnp.int32, (lines, LANES), 1)
    )
    live = row_id < live_count
    total_gap = jnp.sum(jnp.sum(seg_ref[...], axis=0, keepdims=True), axis=1, keepdims=True)
    area_rows = jnp.where(live, jac_ref[...], 0.0)
    total_area = jnp.sum(
        jnp.sum(area_rows, axis=0, keepdims=True), axis=1, keepdims=True
    ) * jnp.sum(qw_ref[...], axis=1, keepdims=True)
    lane = lax.broadcasted_iota(jnp.int32, (1, LANES), 1)
    pair = jnp.where(lane == 0, total_gap, jnp.where(lane == 1, total_area, 0.0))
    tot_s[...] = pair
    tot_d[me] = pair

    def tot_copy(j, source):
        return pltpu.make_async_remote_copy(
            src_ref=tot_s, dst_ref=tot_d.at[source],
            send_sem=s_td.at[j], recv_sem=r_td.at[source],
            device_id=dev(*peer(j)), device_id_type=MESH,
        )

    def start_tot(j, carry):
        tot_copy(j, me).start()
        return carry

    def gather_group(g):
        top, best = scan_group(
            g, 0, DEPTH, code_ref, slot_ref, pen_ref, key_ref,
            (lane_lo, lane_pen, lane_key), accs_pen, accs_key,
        )
        at = pl.ds(g, 1)
        return jnp.maximum(top, over_pen[at, :]), jnp.maximum(best, over_key[at, :])

    def decode(top, best):
        none = top < LOWEST_FILL * 0.5
        rank = jnp.where(none, -1, (best >> 30) + 2)
        face = jnp.where(none, FACE_LIMIT, FACE_MASK - (best & FACE_MASK))
        return rank, face

    spill_f[0] = jnp.full((SUB, LANES), LOWEST_FILL, jnp.float32)
    spill_i[0] = jnp.full((SUB, LANES), -1, jnp.int32)
    spill_i[1] = jnp.full((SUB, LANES), FACE_LIMIT, jnp.int32)
    spill_f[1] = seg_ref[OWN_GROUPS:, :]
    def spill_group(g, carry):
        top, best = gather_group(g)
        rank, face = decode(top, best)
        at = pl.ds(g - OWN_GROUPS, 1)
        spill_f[0, at, :] = top
        spill_i[0, at, :] = rank
        spill_i[1, at, :] = face
        return carry

    lax.fori_loop(OWN_GROUPS, GROUPS, spill_group, 0)

    pl.semaphore_wait(barrier, count - 1)

    lax.fori_loop(1, count, start_tot, 0)

    def spill_copy(j, source):
        return (
            pltpu.make_async_remote_copy(
                src_ref=spill_f, dst_ref=sp_f.at[source],
                send_sem=s_spf.at[j], recv_sem=r_spf.at[source],
                device_id=dev(dom + 1, rep + j), device_id_type=MESH,
            ),
            pltpu.make_async_remote_copy(
                src_ref=spill_i, dst_ref=sp_i.at[source],
                send_sem=s_spi.at[j], recv_sem=r_spi.at[source],
                device_id=dev(dom + 1, rep + j), device_id_type=MESH,
            ),
        )

    for j in range(n_rep):
        for copy in spill_copy(j, rep):
            copy.start()

    own_f[1] = seg_ref[:OWN_GROUPS, :]

    def own_group(g, carry):
        top, best = gather_group(g)
        rank, face = decode(top, best)
        at = pl.ds(g, 1)
        own_f[0, at, :] = top
        own_i[0, at, :] = rank
        own_i[1, at, :] = face
        return carry

    lax.fori_loop(0, OWN_GROUPS, own_group, 0)

    def own_copy(j, source):
        return (
            pltpu.make_async_remote_copy(
                src_ref=own_f, dst_ref=ow_f.at[source],
                send_sem=s_owf.at[j], recv_sem=r_owf.at[source],
                device_id=dev(dom, rep + j), device_id_type=MESH,
            ),
            pltpu.make_async_remote_copy(
                src_ref=own_i, dst_ref=ow_i.at[source],
                send_sem=s_owi.at[j], recv_sem=r_owi.at[source],
                device_id=dev(dom, rep + j), device_id_type=MESH,
            ),
        )

    for j in range(1, n_rep):
        for copy in own_copy(j, rep):
            copy.start()
    ow_f[rep] = own_f[...]
    ow_i[rep] = own_i[...]

    def encode(rank, face):
        return jnp.where(rank < 0, KEY_LOW, ((rank - 2) << 30) + (FACE_MASK - face))

    def wait_tot(j, carry):
        tot_copy(j, lax.rem(me - j + count, count)).wait_recv()
        return carry

    lax.fori_loop(1, count, wait_tot, 0)

    def add_tot(j, total):
        return total + tot_d[j]

    whole = lax.fori_loop(0, count, add_tot, jnp.zeros((1, LANES), jnp.float32))
    out_mean[0] = jnp.sum(whole[:, 0:1]) / jnp.sum(whole[:, 1:2])

    for j in range(n_rep):
        for copy in spill_copy(j, lax.rem(rep - j + n_rep, n_rep)):
            copy.wait_recv()
    pen_s, gap_s = sp_f[0, 0], sp_f[0, 1]
    key_s = encode(sp_i[0, 0], sp_i[0, 1])
    for r in range(1, n_rep):
        pen_s = jnp.maximum(pen_s, sp_f[r, 0])
        gap_s = gap_s + sp_f[r, 1]
        key_s = jnp.maximum(key_s, encode(sp_i[r, 0], sp_i[r, 1]))
    for j in range(1, n_rep):
        for copy in own_copy(j, lax.rem(rep - j + n_rep, n_rep)):
            copy.wait_recv()
    pen_o, key_o, gap_o = pen_s, key_s, ow_f[0, 1]
    for r in range(n_rep):
        pen_o = jnp.maximum(pen_o, ow_f[r, 0])
        key_o = jnp.maximum(key_o, encode(ow_i[r, 0], ow_i[r, 1]))
        if r:
            gap_o = gap_o + ow_f[r, 1]
    out_pen[...] = pen_o
    out_key[...] = key_o
    out_gap[...] = gap_o + gap_s

    def end_tot(j, carry):
        tot_copy(j, me).wait_send()
        return carry

    lax.fori_loop(1, count, end_tot, 0)
    for j in range(1, n_rep):
        for copy in own_copy(j, rep):
            copy.wait_send()
    for j in range(n_rep):
        for copy in spill_copy(j, rep):
            copy.wait_send()


def finish_kernel(pen_ref, key_ref, gap_ref, out_pen, out_face, out_gap):
    none = pen_ref[...] < LOWEST_FILL * 0.5
    out_pen[...] = jnp.where(none, 0.0, pen_ref[...])
    out_face[...] = jnp.where(none, -1, FACE_MASK - (key_ref[...] & FACE_MASK))
    out_gap[...] = jnp.where(none, 0.0, gap_ref[...])


def lane_scratch():
    lane_packs = [
        pltpu.VMEM((DEPTH + SUB, LANES), jnp.int32),
        pltpu.VMEM((DEPTH + SUB, LANES), jnp.float32),
        pltpu.VMEM((DEPTH + SUB, LANES), jnp.int32),
    ]
    lane_accs = [
        pltpu.VMEM((LANES, LANES), jnp.float32),
        pltpu.VMEM((LANES, LANES), jnp.int32),
    ]
    return lane_packs, lane_accs


def dense_call(live, ns, nm, qrow, sec, mst, off, jac, slot, face, rank, block=BLOCK):
    k_size, p_size = ns.shape
    rows = sec.shape[1]
    lines = rows // LANES
    b_lines = block // LANES
    grid = rows // block
    smem = pl.BlockSpec(memory_space=pltpu.SMEM)
    full = lambda shape: pl.BlockSpec(shape, lambda i: (0, 0))
    line_spec = pl.BlockSpec((b_lines, LANES), lambda i: (i, 0))
    wide = pl.BlockSpec((k_size, block), lambda i: (0, i))
    whole = full((lines, LANES))
    padded = full((PAD_GROUPS, LANES))
    lane_packs, lane_accs = lane_scratch()
    return pl.pallas_call(
        dense_kernel,
        grid=(grid,),
        out_shape=(
            jax.ShapeDtypeStruct((k_size, rows), jnp.bfloat16),
            jax.ShapeDtypeStruct((lines, LANES), jnp.float32),
            jax.ShapeDtypeStruct((PAD_GROUPS, LANES), jnp.float32),
            jax.ShapeDtypeStruct((lines, LANES), jnp.int32),
            jax.ShapeDtypeStruct((lines, LANES), jnp.int32),
            jax.ShapeDtypeStruct((PAD_GROUPS, LANES), jnp.float32),
            jax.ShapeDtypeStruct((PAD_GROUPS, LANES), jnp.int32),
        ),
        in_specs=[
            smem, full((k_size, p_size)), full((k_size, p_size)), full((1, p_size)),
            wide, wide, line_spec, line_spec, whole, whole, whole,
        ],
        out_specs=(wide, whole, padded, whole, whole, padded, padded),
        scratch_shapes=[
            pltpu.VMEM((p_size + 16, 2 * k_size + 16), jnp.bfloat16),
            pltpu.VMEM((2 * k_size, p_size), jnp.bfloat16),
            lane_packs,
            *lane_accs,
        ],
        compiler_params=pltpu.CompilerParams(dimension_semantics=("arbitrary",)),
    )(live, ns, nm, qrow, sec, mst, off, jac, slot, face, rank)


def solution(mesh):
    n_dom, n_rep = mesh.shape["dom"], mesh.shape["rep"]

    def shards(ns, nm, sec, mst, off, qw, jac, slot, face, rank, live):
        k_size, p_size = ns.shape
        rows = sec.shape[1]
        lines = rows // LANES

        def lined(x):
            return x.reshape(lines, LANES)

        qrow = qw.reshape(1, p_size)
        off, jac, slot, face, rank = (lined(x) for x in (off, jac, slot, face, rank))
        smem = pl.BlockSpec(memory_space=pltpu.SMEM)
        lane_packs, lane_accs = lane_scratch()
        force, pen, seg, code, key, over_pen, over_key = dense_call(
            live, ns, nm, qrow, sec, mst, off, jac, slot, face, rank
        )

        vmem = pl.BlockSpec(memory_space=pltpu.VMEM)
        tile_f = (2, SUB, LANES)
        sems = pltpu.SemaphoreType.DMA
        best_pen, best_key, gap_sum, mean = pl.pallas_call(
            functools.partial(merge_kernel, n_dom, n_rep),
            out_shape=(
                jax.ShapeDtypeStruct((SUB, LANES), jnp.float32),
                jax.ShapeDtypeStruct((SUB, LANES), jnp.int32),
                jax.ShapeDtypeStruct((SUB, LANES), jnp.float32),
                jax.ShapeDtypeStruct((1,), jnp.float32),
            ),
            in_specs=[smem, vmem] + [pl.BlockSpec(memory_space=pl.ANY)] * 8,
            out_specs=(vmem, vmem, vmem, smem),
            scratch_shapes=[
                pltpu.VMEM((lines, LANES), jnp.int32),
                pltpu.VMEM((lines, LANES), jnp.int32),
                pltpu.VMEM((lines, LANES), jnp.int32),
                pltpu.VMEM((lines, LANES), jnp.float32),
                pltpu.VMEM((lines, LANES), jnp.float32),
                pltpu.VMEM((PAD_GROUPS, LANES), jnp.float32),
                pltpu.VMEM((PAD_GROUPS, LANES), jnp.float32),
                pltpu.VMEM((PAD_GROUPS, LANES), jnp.int32),
                sems((8,)),
                *lane_packs,
                *lane_accs,
                pltpu.VMEM((n_rep,) + tile_f, jnp.float32),
                pltpu.VMEM((n_rep,) + tile_f, jnp.int32),
                pltpu.VMEM((n_rep,) + tile_f, jnp.float32),
                pltpu.VMEM((n_rep,) + tile_f, jnp.int32),
                pltpu.VMEM((n_dom * n_rep, 1, LANES), jnp.float32),
                pltpu.VMEM((1, LANES), jnp.float32),
                pltpu.VMEM(tile_f, jnp.float32),
                pltpu.VMEM(tile_f, jnp.int32),
                pltpu.VMEM(tile_f, jnp.float32),
                pltpu.VMEM(tile_f, jnp.int32),
                sems((n_rep,)), sems((n_rep,)), sems((n_rep,)), sems((n_rep,)),
                sems((n_rep,)), sems((n_rep,)), sems((n_rep,)), sems((n_rep,)),
                sems((n_dom * n_rep,)), sems((n_dom * n_rep,)),
            ],
            compiler_params=pltpu.CompilerParams(collective_id=0, has_side_effects=True),
        )(live, qrow, slot, code, key, pen, jac, seg, over_pen, over_key)
        seg_pen, seg_face, seg_gap = pl.pallas_call(
            finish_kernel,
            out_shape=(
                jax.ShapeDtypeStruct((SUB, LANES), jnp.float32),
                jax.ShapeDtypeStruct((SUB, LANES), jnp.int32),
                jax.ShapeDtypeStruct((SUB, LANES), jnp.float32),
            ),
            in_specs=[vmem] * 3,
            out_specs=(vmem, vmem, vmem),
        )(best_pen, best_key, gap_sum)
        seg_pen, seg_face, seg_gap = (x.reshape(SEG_DEV) for x in (seg_pen, seg_face, seg_gap))
        return force, seg_pen, seg_face, seg_gap, mean.reshape(())

    return jax.shard_map(
        shards,
        mesh=mesh,
        in_specs=(
            P(),
            P(),
            P(None, ("dom", "rep")),
            P(None, ("dom", "rep")),
            P(("dom", "rep")),
            P(),
            P(("dom", "rep")),
            P(("dom", "rep")),
            P(("dom", "rep")),
            P(("dom", "rep")),
            P(("dom", "rep")),
        ),
        out_specs=(P(None, ("dom", "rep")), P("dom"), P("dom"), P("dom"), P()),
        check_vma=False,
    )
```

```python
import functools

import jax
import jax.numpy as jnp
from jax import lax
from jax.experimental import pallas as pl
from jax.experimental.pallas import tpu as pltpu
from jax.sharding import PartitionSpec as P

SEG_DEV = 1024
SPILL = 256
LANES = 128
SUB = 8
GROUPS = (SEG_DEV + SPILL) // LANES
OWN_GROUPS = SEG_DEV // LANES
PAD_GROUPS = 16

PENALTY = 400.0
LOWEST_FILL = -1e30
FACE_LIMIT = 1073741824
FACE_MASK = FACE_LIMIT - 1
KEY_LOW = -2147483648
MESH = pl.DeviceIdType.MESH
TILE = 256
DEPTH = 16
BLOCK = 4096


def split3(x):
    a = x.astype(jnp.bfloat16)
    rest = x - a.astype(jnp.float32)
    b = rest.astype(jnp.bfloat16)
    c = (rest - b.astype(jnp.float32)).astype(jnp.bfloat16)
    return a, b, c


def scan_group(g, depth0, depth, code_ref, slot_ref, pen_ref, key_ref, packs, accs_pen, accs_key):
    all_lines = code_ref.shape[0]
    lane_lo, lane_pen, lane_key = packs
    blocks = depth // SUB
    sub = lax.broadcasted_iota(jnp.int32, (SUB, LANES), 0)
    wants = [(sub + (depth0 + SUB * b)) * PAD_GROUPS + g for b in range(blocks)]

    def pull(i, carry):
        los, pens, keys = (list(part) for part in carry)
        code = code_ref[pl.ds(i, SUB, stride=0), :]
        slot = slot_ref[pl.ds(i, SUB, stride=0), :]
        pen = pen_ref[pl.ds(i, SUB, stride=0), :]
        key = key_ref[pl.ds(i, SUB, stride=0), :]
        for b in range(blocks):
            hit = code == wants[b]
            los[b] = jnp.where(hit, slot, los[b])
            pens[b] = jnp.where(hit, pen, pens[b])
            keys[b] = jnp.where(hit, key, keys[b])
        return tuple(los), tuple(pens), tuple(keys)

    none = jnp.full((SUB, LANES), -1, jnp.int32)
    empty = jnp.full((SUB, LANES), LOWEST_FILL, jnp.float32)
    start = ((none,) * blocks, (empty,) * blocks, (none,) * blocks)
    los, pens, keys = lax.fori_loop(0, all_lines, pull, start, unroll=8)
    for b in range(blocks):
        rows = slice(SUB * b, SUB * (b + 1))
        lane_lo[rows, :] = los[b]
        lane_pen[rows, :] = pens[b]
        lane_key[rows, :] = keys[b]

    tiles = LANES // SUB
    half = tiles // 2
    for part in range(2):
        marks = [sub + (g * LANES + SUB * (part * half + q)) for q in range(half)]
        best_pen = [empty] * half
        best_key = [jnp.full((SUB, LANES), KEY_LOW, jnp.int32)] * half
        for j in range(depth):
            lo = lane_lo[pl.ds(j, SUB, stride=0), :]
            pen = lane_pen[pl.ds(j, SUB, stride=0), :]
            key = lane_key[pl.ds(j, SUB, stride=0), :]
            for q in range(half):
                hit = lo == marks[q]
                best_pen[q] = jnp.maximum(best_pen[q], jnp.where(hit, pen, LOWEST_FILL))
                best_key[q] = jnp.maximum(best_key[q], jnp.where(hit, key, KEY_LOW))
        for q in range(half):
            rows = slice(SUB * (part * half + q), SUB * (part * half + q + 1))
            accs_pen[rows, :] = best_pen[q]
            accs_key[rows, :] = best_key[q]
    top = jnp.max(accs_pen[...].T, axis=0, keepdims=True)
    best = jnp.max(accs_key[...].T, axis=0, keepdims=True)
    return top, best


def dense_kernel(
    live_ref, ns_ref, nm_ref, qw_ref, sec_ref, mst_ref, off_ref, jac_ref, slot_ref,
    face_ref, rank_ref,
    force_ref, pen_ref, gap_ref, code_ref, key_ref, over_pen, over_key,
    wt_ref, nq_ref, packs, accs_pen, accs_key,
):
    step = pl.program_id(0)
    all_lines = slot_ref.shape[0]
    k_size, p_size = ns_ref.shape
    rows = sec_ref.shape[1]
    lines = rows // LANES
    per_tile = TILE // LANES

    @pl.when(step == 0)
    def _():
        w = jnp.concatenate([ns_ref[...], -nm_ref[...]], axis=0).astype(jnp.float32)
        qrow = qw_ref[...]
        wt = w.T
        qmat = jnp.broadcast_to(qrow, (LANES, p_size)).T
        v = jnp.sum(wt * qmat, axis=0, keepdims=True)
        qsum = jnp.sum(qmat, axis=0, keepdims=True)
        depth = wt_ref.shape[1]
        pick = lax.broadcasted_iota(jnp.int32, (16, depth), 0)
        column = lax.broadcasted_iota(jnp.int32, (p_size, depth - 2 * k_size), 1)
        wt_ref[0:p_size, 0 : 2 * k_size] = wt.astype(jnp.bfloat16)
        wt_ref[0:p_size, 2 * k_size :] = jnp.where(column < 3, 1.0, 0.0).astype(jnp.bfloat16)
        lane_row = lax.broadcasted_iota(jnp.int32, (1, LANES), 1)
        tail = jnp.where(lane_row < 3, qsum, 0.0)[:, : depth - 2 * k_size]
        a, b, c = (part.astype(jnp.float32) for part in split3(jnp.concatenate([v, tail], axis=1)))
        stacked = jnp.where(
            pick == 0, a, jnp.where(pick == 1, b, jnp.where(pick == 2, c, 0.0))
        )
        wt_ref[p_size:, :] = stacked.astype(jnp.bfloat16)
        scaled = ns_ref[...].astype(jnp.float32) * qrow
        top = scaled.astype(jnp.bfloat16)
        low = (scaled - top.astype(jnp.float32)).astype(jnp.bfloat16)
        nq_ref[...] = jnp.concatenate([top, low], axis=0)
        over_pen[...] = jnp.full(over_pen.shape, LOWEST_FILL, jnp.float32)
        over_key[...] = jnp.full(over_key.shape, KEY_LOW, jnp.int32)
        row_id = (
            lax.broadcasted_iota(jnp.int32, (all_lines, LANES), 0) * LANES
            + lax.broadcasted_iota(jnp.int32, (all_lines, LANES), 1)
        )
        alive = row_id < live_ref[0]
        key_ref[...] = ((rank_ref[...] - 2) << 30) + (FACE_MASK - face_ref[...])
        group = jnp.where(alive, slot_ref[...] >> 7, -1)
        before = (
            lax.broadcasted_iota(jnp.int32, (all_lines, all_lines), 1)
            < lax.broadcasted_iota(jnp.int32, (all_lines, all_lines), 0)
        )
        before = jnp.where(before, 1.0, 0.0).astype(jnp.bfloat16)
        code = jnp.full((all_lines, LANES), -1, jnp.int32)
        for g in range(GROUPS):
            mine = group == g
            place = jnp.dot(
                before, jnp.where(mine, 1.0, 0.0).astype(jnp.bfloat16),
                preferred_element_type=jnp.float32,
            ).astype(jnp.int32)
            code = jnp.where(mine, place * PAD_GROUPS + g, code)
        code_ref[...] = code

    live_count = live_ref[0]
    first = step * rows
    line0 = step * lines
    wt = wt_ref[...]
    nq = nq_ref[...]
    pad_rows = wt.shape[1] - 2 * k_size
    pad_id = lax.broadcasted_iota(jnp.int32, (pad_rows, TILE), 0)

    def line_of(ref, at, count):
        return jnp.concatenate([ref[pl.ds(at + i, 1), :] for i in range(count)], axis=1)

    def project(tile):
        cols = pl.ds(tile * TILE, TILE)
        offset = line_of(off_ref, tile * per_tile, per_tile)
        a, b, c = (part.astype(jnp.float32) for part in split3(offset))
        extra = jnp.where(pad_id == 0, a, jnp.where(pad_id == 1, b, jnp.where(pad_id == 2, c, 0.0)))
        x = jnp.concatenate([sec_ref[:, cols], mst_ref[:, cols], extra.astype(jnp.bfloat16)], axis=0)
        return jnp.dot(wt, x, preferred_element_type=jnp.float32)

    row_lane = lax.broadcasted_iota(jnp.int32, (1, TILE), 1)
    tiles = rows // TILE
    field = project(0)
    for tile in range(tiles):
        cols = pl.ds(tile * TILE, TILE)
        coming = project(tile + 1) if tile + 1 < tiles else None
        gap = field[:p_size]
        live = (row_lane + (first + tile * TILE)) < live_count
        jac_live = jnp.where(live, line_of(jac_ref, tile * per_tile, per_tile), 0.0)
        load = jnp.minimum(gap.astype(jnp.bfloat16), 0)
        force = jnp.dot(nq, load, preferred_element_type=jnp.float32)
        force_ref[:, cols] = (
            (force[:k_size] + force[k_size:]) * (jac_live * -PENALTY)
        ).astype(jnp.bfloat16)
        pen = jnp.where(live, -jnp.min(gap, axis=0, keepdims=True), LOWEST_FILL)
        for part in range(per_tile):
            pen_ref[pl.ds(line0 + tile * per_tile + part, 1), :] = pen[:, part * LANES : (part + 1) * LANES]
        row_gap = jac_live * jnp.sum(field[p_size : p_size + SUB], axis=0, keepdims=True)
        for part in range(per_tile):
            gap_ref[pl.ds(line0 + tile * per_tile + part, 1), :] = row_gap[:, part * LANES : (part + 1) * LANES]
        field = coming
    @pl.when(step == pl.num_programs(0) - 1)
    def _():
        def one(worst):
            code = code_ref[...]
            g = worst & (PAD_GROUPS - 1)
            low = (worst >> 4) & -SUB
            top, best = scan_group(
                g, low, SUB, code_ref, slot_ref, pen_ref, key_ref, packs, accs_pen, accs_key
            )
            at = pl.ds(g, 1)
            over_pen[at, :] = jnp.maximum(over_pen[at, :], top)
            over_key[at, :] = jnp.maximum(over_key[at, :], best)
            done = ((code & (PAD_GROUPS - 1)) == g) & (code >= low * PAD_GROUPS)
            code = jnp.where(done, -1, code)
            code_ref[...] = code
            return jnp.max(code)

        lax.while_loop(lambda worst: worst >= DEPTH * PAD_GROUPS, one, jnp.max(code_ref[...]))


def merge_kernel(
    n_dom, n_rep,
    live_ref, qw_ref, slot_h, code_h, key_h, pen_h, jac_h, gap_h, over_pen_h, over_key_h,
    out_pen, out_key, out_gap, out_mean,
    slot_ref, code_ref, key_ref, pen_ref, jac_ref, gap_ref, over_pen, over_key, s_in, seg_ref,
    lane_lo, lane_pen, lane_key, accs_pen, accs_key,
    sp_f, sp_i, ow_f, ow_i, tot_d, tot_s,
    spill_f, spill_i, own_f, own_i,
    s_spf, r_spf, s_spi, r_spi, s_owf, r_owf, s_owi, r_owi, s_td, r_td,
):
    dom = lax.axis_index("dom")
    rep = lax.axis_index("rep")
    lines = slot_ref.shape[0]

    def dev(d, r):
        return {"dom": lax.rem(d + n_dom, n_dom), "rep": lax.rem(r + n_rep, n_rep)}

    barrier = pltpu.get_barrier_semaphore()

    def greet(d, r):
        pl.semaphore_signal(barrier, inc=1, device_id=dev(d, r), device_id_type=MESH)

    count = n_dom * n_rep
    me = dom * n_rep + rep

    def peer(j):
        flat = lax.rem(me + j, count)
        return lax.div(flat, n_rep), lax.rem(flat, n_rep)

    def greet_peer(j, carry):
        greet(*peer(j))
        return carry

    lax.fori_loop(1, count, greet_peer, 0)
    loads = [
        pltpu.make_async_copy(source, held, s_in.at[i])
        for i, (source, held) in enumerate((
            (slot_h, slot_ref), (code_h, code_ref), (key_h, key_ref), (pen_h, pen_ref),
            (jac_h, jac_ref), (gap_h, gap_ref), (over_pen_h, over_pen), (over_key_h, over_key),
        ))
    ]
    for copy in loads:
        copy.start()
    for copy in loads:
        copy.wait()

    live_count = live_ref[0]
    row_id = (
        lax.broadcasted_iota(jnp.int32, (lines, LANES), 0) * LANES
        + lax.broadcasted_iota(jnp.int32, (lines, LANES), 1)
    )
    live = row_id < live_count
    total_gap = jnp.sum(jnp.sum(gap_ref[...], axis=0, keepdims=True), axis=1, keepdims=True)
    area_rows = jnp.where(live, jac_ref[...], 0.0)
    total_area = jnp.sum(
        jnp.sum(area_rows, axis=0, keepdims=True), axis=1, keepdims=True
    ) * jnp.sum(qw_ref[...], axis=1, keepdims=True)
    lane = lax.broadcasted_iota(jnp.int32, (1, LANES), 1)
    pair = jnp.where(lane == 0, total_gap, jnp.where(lane == 1, total_area, 0.0))
    tot_s[...] = pair
    tot_d[me] = pair

    def tot_copy(j, source):
        return pltpu.make_async_remote_copy(
            src_ref=tot_s, dst_ref=tot_d.at[source],
            send_sem=s_td.at[j], recv_sem=r_td.at[source],
            device_id=dev(*peer(j)), device_id_type=MESH,
        )

    def start_tot(j, carry):
        tot_copy(j, me).start()
        return carry

    hi_id = lax.broadcasted_iota(jnp.int32, (PAD_GROUPS, LANES), 0)
    lo_id = lax.broadcasted_iota(jnp.int32, (LANES, LANES), 0)

    def add_gaps(turn, total):
        lefts, rights = [], []
        for i in range(SUB):
            at = pl.ds(turn * SUB + i, 1)
            slot = slot_ref[at, :]
            lefts.append(jnp.where(hi_id == (slot >> 7), gap_ref[at, :], 0.0))
            rights.append(jnp.where(lo_id == (slot & (LANES - 1)), 1.0, 0.0).astype(jnp.bfloat16))
        left = jnp.concatenate(split3(jnp.concatenate(lefts, axis=1)), axis=0)
        got = lax.dot_general(
            left, jnp.concatenate(rights, axis=1), (((1,), (1,)), ((), ())),
            preferred_element_type=jnp.float32,
        )
        return total + (got[0:PAD_GROUPS] + got[PAD_GROUPS : 2 * PAD_GROUPS] + got[2 * PAD_GROUPS :])

    zero = jnp.zeros((PAD_GROUPS, LANES), jnp.float32)
    seg_ref[...] = lax.fori_loop(0, lines // SUB, add_gaps, zero)

    def gather_group(g):
        top, best = scan_group(
            g, 0, DEPTH, code_ref, slot_ref, pen_ref, key_ref,
            (lane_lo, lane_pen, lane_key), accs_pen, accs_key,
        )
        at = pl.ds(g, 1)
        return jnp.maximum(top, over_pen[at, :]), jnp.maximum(best, over_key[at, :])

    def decode(top, best):
        none = top < LOWEST_FILL * 0.5
        rank = jnp.where(none, -1, (best >> 30) + 2)
        face = jnp.where(none, FACE_LIMIT, FACE_MASK - (best & FACE_MASK))
        return rank, face

    spill_f[0] = jnp.full((SUB, LANES), LOWEST_FILL, jnp.float32)
    spill_i[0] = jnp.full((SUB, LANES), -1, jnp.int32)
    spill_i[1] = jnp.full((SUB, LANES), FACE_LIMIT, jnp.int32)
    spill_f[1] = seg_ref[OWN_GROUPS:, :]
    def spill_group(g, carry):
        top, best = gather_group(g)
        rank, face = decode(top, best)
        at = pl.ds(g - OWN_GROUPS, 1)
        spill_f[0, at, :] = top
        spill_i[0, at, :] = rank
        spill_i[1, at, :] = face
        return carry

    lax.fori_loop(OWN_GROUPS, GROUPS, spill_group, 0)

    pl.semaphore_wait(barrier, count - 1)

    lax.fori_loop(1, count, start_tot, 0)

    def spill_copy(j, source):
        return (
            pltpu.make_async_remote_copy(
                src_ref=spill_f, dst_ref=sp_f.at[source],
                send_sem=s_spf.at[j], recv_sem=r_spf.at[source],
                device_id=dev(dom + 1, rep + j), device_id_type=MESH,
            ),
            pltpu.make_async_remote_copy(
                src_ref=spill_i, dst_ref=sp_i.at[source],
                send_sem=s_spi.at[j], recv_sem=r_spi.at[source],
                device_id=dev(dom + 1, rep + j), device_id_type=MESH,
            ),
        )

    for j in range(n_rep):
        for copy in spill_copy(j, rep):
            copy.start()

    own_f[1] = seg_ref[:OWN_GROUPS, :]

    def own_group(g, carry):
        top, best = gather_group(g)
        rank, face = decode(top, best)
        at = pl.ds(g, 1)
        own_f[0, at, :] = top
        own_i[0, at, :] = rank
        own_i[1, at, :] = face
        return carry

    lax.fori_loop(0, OWN_GROUPS, own_group, 0)

    def own_copy(j, source):
        return (
            pltpu.make_async_remote_copy(
                src_ref=own_f, dst_ref=ow_f.at[source],
                send_sem=s_owf.at[j], recv_sem=r_owf.at[source],
                device_id=dev(dom, rep + j), device_id_type=MESH,
            ),
            pltpu.make_async_remote_copy(
                src_ref=own_i, dst_ref=ow_i.at[source],
                send_sem=s_owi.at[j], recv_sem=r_owi.at[source],
                device_id=dev(dom, rep + j), device_id_type=MESH,
            ),
        )

    for j in range(1, n_rep):
        for copy in own_copy(j, rep):
            copy.start()
    ow_f[rep] = own_f[...]
    ow_i[rep] = own_i[...]

    def encode(rank, face):
        return jnp.where(rank < 0, KEY_LOW, ((rank - 2) << 30) + (FACE_MASK - face))

    def wait_tot(j, carry):
        tot_copy(j, lax.rem(me - j + count, count)).wait_recv()
        return carry

    lax.fori_loop(1, count, wait_tot, 0)

    def add_tot(j, total):
        return total + tot_d[j]

    whole = lax.fori_loop(0, count, add_tot, jnp.zeros((1, LANES), jnp.float32))
    out_mean[0] = jnp.sum(whole[:, 0:1]) / jnp.sum(whole[:, 1:2])

    for j in range(n_rep):
        for copy in spill_copy(j, lax.rem(rep - j + n_rep, n_rep)):
            copy.wait_recv()
    pen_s, gap_s = sp_f[0, 0], sp_f[0, 1]
    key_s = encode(sp_i[0, 0], sp_i[0, 1])
    for r in range(1, n_rep):
        pen_s = jnp.maximum(pen_s, sp_f[r, 0])
        gap_s = gap_s + sp_f[r, 1]
        key_s = jnp.maximum(key_s, encode(sp_i[r, 0], sp_i[r, 1]))
    for j in range(1, n_rep):
        for copy in own_copy(j, lax.rem(rep - j + n_rep, n_rep)):
            copy.wait_recv()
    pen_o, key_o, gap_o = pen_s, key_s, ow_f[0, 1]
    for r in range(n_rep):
        pen_o = jnp.maximum(pen_o, ow_f[r, 0])
        key_o = jnp.maximum(key_o, encode(ow_i[r, 0], ow_i[r, 1]))
        if r:
            gap_o = gap_o + ow_f[r, 1]
    out_pen[...] = pen_o
    out_key[...] = key_o
    out_gap[...] = gap_o + gap_s

    def end_tot(j, carry):
        tot_copy(j, me).wait_send()
        return carry

    lax.fori_loop(1, count, end_tot, 0)
    for j in range(1, n_rep):
        for copy in own_copy(j, rep):
            copy.wait_send()
    for j in range(n_rep):
        for copy in spill_copy(j, rep):
            copy.wait_send()


def finish_kernel(pen_ref, key_ref, gap_ref, out_pen, out_face, out_gap):
    none = pen_ref[...] < LOWEST_FILL * 0.5
    out_pen[...] = jnp.where(none, 0.0, pen_ref[...])
    out_face[...] = jnp.where(none, -1, FACE_MASK - (key_ref[...] & FACE_MASK))
    out_gap[...] = jnp.where(none, 0.0, gap_ref[...])


def lane_scratch():
    lane_packs = [
        pltpu.VMEM((DEPTH + SUB, LANES), jnp.int32),
        pltpu.VMEM((DEPTH + SUB, LANES), jnp.float32),
        pltpu.VMEM((DEPTH + SUB, LANES), jnp.int32),
    ]
    lane_accs = [
        pltpu.VMEM((LANES, LANES), jnp.float32),
        pltpu.VMEM((LANES, LANES), jnp.int32),
    ]
    return lane_packs, lane_accs


def dense_call(live, ns, nm, qrow, sec, mst, off, jac, slot, face, rank, block=BLOCK):
    k_size, p_size = ns.shape
    rows = sec.shape[1]
    lines = rows // LANES
    b_lines = block // LANES
    grid = rows // block
    smem = pl.BlockSpec(memory_space=pltpu.SMEM)
    full = lambda shape: pl.BlockSpec(shape, lambda i: (0, 0))
    line_spec = pl.BlockSpec((b_lines, LANES), lambda i: (i, 0))
    wide = pl.BlockSpec((k_size, block), lambda i: (0, i))
    whole = full((lines, LANES))
    padded = full((PAD_GROUPS, LANES))
    lane_packs, lane_accs = lane_scratch()
    return pl.pallas_call(
        dense_kernel,
        grid=(grid,),
        out_shape=(
            jax.ShapeDtypeStruct((k_size, rows), jnp.bfloat16),
            jax.ShapeDtypeStruct((lines, LANES), jnp.float32),
            jax.ShapeDtypeStruct((lines, LANES), jnp.float32),
            jax.ShapeDtypeStruct((lines, LANES), jnp.int32),
            jax.ShapeDtypeStruct((lines, LANES), jnp.int32),
            jax.ShapeDtypeStruct((PAD_GROUPS, LANES), jnp.float32),
            jax.ShapeDtypeStruct((PAD_GROUPS, LANES), jnp.int32),
        ),
        in_specs=[
            smem, full((k_size, p_size)), full((k_size, p_size)), full((1, p_size)),
            wide, wide, line_spec, line_spec, whole, whole, whole,
        ],
        out_specs=(wide, whole, whole, whole, whole, padded, padded),
        scratch_shapes=[
            pltpu.VMEM((p_size + 16, 2 * k_size + 16), jnp.bfloat16),
            pltpu.VMEM((2 * k_size, p_size), jnp.bfloat16),
            lane_packs,
            *lane_accs,
        ],
        compiler_params=pltpu.CompilerParams(dimension_semantics=("arbitrary",)),
    )(live, ns, nm, qrow, sec, mst, off, jac, slot, face, rank)


def solution(mesh):
    n_dom, n_rep = mesh.shape["dom"], mesh.shape["rep"]

    def shards(ns, nm, sec, mst, off, qw, jac, slot, face, rank, live):
        k_size, p_size = ns.shape
        rows = sec.shape[1]
        lines = rows // LANES

        def lined(x):
            return x.reshape(lines, LANES)

        qrow = qw.reshape(1, p_size)
        off, jac, slot, face, rank = (lined(x) for x in (off, jac, slot, face, rank))
        smem = pl.BlockSpec(memory_space=pltpu.SMEM)
        lane_packs, lane_accs = lane_scratch()
        force, pen, gap, code, key, over_pen, over_key = dense_call(
            live, ns, nm, qrow, sec, mst, off, jac, slot, face, rank
        )

        vmem = pl.BlockSpec(memory_space=pltpu.VMEM)
        tile_f = (2, SUB, LANES)
        sems = pltpu.SemaphoreType.DMA
        best_pen, best_key, gap_sum, mean = pl.pallas_call(
            functools.partial(merge_kernel, n_dom, n_rep),
            out_shape=(
                jax.ShapeDtypeStruct((SUB, LANES), jnp.float32),
                jax.ShapeDtypeStruct((SUB, LANES), jnp.int32),
                jax.ShapeDtypeStruct((SUB, LANES), jnp.float32),
                jax.ShapeDtypeStruct((1,), jnp.float32),
            ),
            in_specs=[smem, vmem] + [pl.BlockSpec(memory_space=pl.ANY)] * 8,
            out_specs=(vmem, vmem, vmem, smem),
            scratch_shapes=[
                pltpu.VMEM((lines, LANES), jnp.int32),
                pltpu.VMEM((lines, LANES), jnp.int32),
                pltpu.VMEM((lines, LANES), jnp.int32),
                pltpu.VMEM((lines, LANES), jnp.float32),
                pltpu.VMEM((lines, LANES), jnp.float32),
                pltpu.VMEM((lines, LANES), jnp.float32),
                pltpu.VMEM((PAD_GROUPS, LANES), jnp.float32),
                pltpu.VMEM((PAD_GROUPS, LANES), jnp.int32),
                sems((8,)),
                pltpu.VMEM((PAD_GROUPS, LANES), jnp.float32),
                *lane_packs,
                *lane_accs,
                pltpu.VMEM((n_rep,) + tile_f, jnp.float32),
                pltpu.VMEM((n_rep,) + tile_f, jnp.int32),
                pltpu.VMEM((n_rep,) + tile_f, jnp.float32),
                pltpu.VMEM((n_rep,) + tile_f, jnp.int32),
                pltpu.VMEM((n_dom * n_rep, 1, LANES), jnp.float32),
                pltpu.VMEM((1, LANES), jnp.float32),
                pltpu.VMEM(tile_f, jnp.float32),
                pltpu.VMEM(tile_f, jnp.int32),
                pltpu.VMEM(tile_f, jnp.float32),
                pltpu.VMEM(tile_f, jnp.int32),
                sems((n_rep,)), sems((n_rep,)), sems((n_rep,)), sems((n_rep,)),
                sems((n_rep,)), sems((n_rep,)), sems((n_rep,)), sems((n_rep,)),
                sems((n_dom * n_rep,)), sems((n_dom * n_rep,)),
            ],
            compiler_params=pltpu.CompilerParams(collective_id=0, has_side_effects=True),
        )(live, qrow, slot, code, key, pen, jac, gap, over_pen, over_key)
        seg_pen, seg_face, seg_gap = pl.pallas_call(
            finish_kernel,
            out_shape=(
                jax.ShapeDtypeStruct((SUB, LANES), jnp.float32),
                jax.ShapeDtypeStruct((SUB, LANES), jnp.int32),
                jax.ShapeDtypeStruct((SUB, LANES), jnp.float32),
            ),
            in_specs=[vmem] * 3,
            out_specs=(vmem, vmem, vmem),
        )(best_pen, best_key, gap_sum)
        seg_pen, seg_face, seg_gap = (x.reshape(SEG_DEV) for x in (seg_pen, seg_face, seg_gap))
        return force, seg_pen, seg_face, seg_gap, mean.reshape(())

    return jax.shard_map(
        shards,
        mesh=mesh,
        in_specs=(
            P(),
            P(),
            P(None, ("dom", "rep")),
            P(None, ("dom", "rep")),
            P(("dom", "rep")),
            P(),
            P(("dom", "rep")),
            P(("dom", "rep")),
            P(("dom", "rep")),
            P(("dom", "rep")),
            P(("dom", "rep")),
        ),
        out_specs=(P(None, ("dom", "rep")), P("dom"), P("dom"), P("dom"), P()),
        check_vma=False,
    )
```
